32 devices in a mesh: seq: 4 (over x, core), wide: 8 (over z, y).
Axes of the slice: x: 2, y: 2, z: 4, core: 2. Of those that a mesh axis runs over, the one named last changes fastest.
Arguments:
- images: bfloat16 [8, 1028, 768], P('wide', 'seq'), may hold values from -6 to 6
- cotangent: bfloat16 [8, 1028, 768], P('wide', 'seq'), may hold values from -6 to 6
- key_mask: int32 [8, 1028], P('wide'), may hold values from 0 to 1, as said below
- routes: int32 [8, 1028, 2], P('wide', 'seq'), may hold values from 0 to 3, all different within a row
- fill_order: int32 [8, 1028], P('wide', 'seq'), may hold values from 0 to 256, as said below
- norm_gain1: bfloat16 [768], P('wide'), may hold values from 0.099609375 to 1.8984375
- qkv_weight1: bfloat16 [768, 2304], P('wide'), may hold values from -0.21875 to 0.21875
- proj_weight1: bfloat16 [768, 768], P('wide'), may hold values from -6 to 6
- norm_gain2: bfloat16 [768], P('wide'), may hold values from 0.099609375 to 1.8984375
- fc_in: bfloat16 [768, 3072], P('wide'), may hold values from -0.21875 to 0.21875
- fc_out: bfloat16 [3072, 768], P('wide'), may hold values from -0.109375 to 0.109375
- norm_gain3: bfloat16 [768], P('wide'), may hold values from 0.099609375 to 1.8984375
- qkv_weight2: bfloat16 [768, 2304], P('wide'), may hold values from -0.21875 to 0.21875
- proj_weight2: bfloat16 [768, 768], P('wide'), may hold values from -6 to 6
- norm_gain4: bfloat16 [768], P('wide'), may hold values from 0.099609375 to 1.8984375
- router: bfloat16 [768, 4], P('wide'), may hold values from -0.21875 to 0.21875
- expert_in: bfloat16 [8, 768, 1536], P('wide'), may hold values from -0.21875 to 0.21875
- expert_out: bfloat16 [8, 1536, 768], P('wide'), may hold values from -3.5 to 3.5
Outputs:
- output: float32 [8, 1028, 768], P('wide', 'seq')
- image_grad: float32 [8, 1028, 768], P('wide', 'seq')
- norm_gain1_grad: float32 [768], P('wide')
- qkv_weight1_grad: float32 [768, 2304], P('wide')
- proj_weight1_grad: float32 [768, 768], P('wide')
- norm_gain2_grad: float32 [768], P('wide')
- fc_in_grad: float32 [768, 3072], P('wide')
- fc_out_grad: float32 [3072, 768], P('wide')
- norm_gain3_grad: float32 [768], P('wide')
- qkv_weight2_grad: float32 [768, 2304], P('wide')
- proj_weight2_grad: float32 [768, 768], P('wide')
- norm_gain4_grad: float32 [768], P('wide')
- router_grad: float32 [768, 4], P('wide')
- expert_in_grad: float32 [8, 768, 1536], P('wide')
- expert_out_grad: float32 [8, 1536, 768], P('wide')
The draws below stay inside these ranges and needn't reach their ends.
Inputs may be any that keep to these rules, and one draw needn't show every extreme that they name: `key_mask`: position 0 of every image is 1. The two routes of a token differ. `fill_order`: in each image, each aligned block of 257 positions holds every number from 0 to 256 once.
All inputs are finite; a program needn't handle non-finite values.
Results may differ from the reference program's by a relative error of at most 0.02.
Values may be sent and summed in bfloat16 or wider, within the bound.
A program may use at most 256 MiB of HBM per device.

```python
import jax
import jax.numpy as jnp
from jax import lax

D = 768
HEADS = 12
HEAD_DIM = 64
FF = 3072
FE = 3072
LENGTH = 1028
EXPERTS = 4
IMAGES = 8
TOK_DEV = 257
CAPACITY = 161
N_SEQ = 4


def draw_key_mask(key, part):
    random_bits = jax.random.randint(key, (IMAGES, LENGTH), 0, 4)
    leading = jnp.arange(LENGTH)[None, :] == 0
    return jnp.where(leading | (random_bits > 0), 1, 0).astype(jnp.int32)


def draw_fill_order(key, part):
    block_count = IMAGES * (LENGTH // TOK_DEV)
    block_keys = jax.random.split(key, block_count)
    orders = jax.vmap(lambda one_key: jax.random.permutation(one_key, TOK_DEV))(block_keys)
    return orders.reshape(IMAGES, LENGTH).astype(jnp.int32)


def levels(rng, extent, cuts, low, top_value):
    level, own = 1.0, jax.random.fold_in(rng, 6)
    for axis_at, shards_of in cuts:
        steps = jnp.exp(jax.random.uniform(jax.random.fold_in(own, axis_at), (shards_of,), jnp.float32, low / len(cuts), top_value / len(cuts)))
        level = level * jnp.repeat(steps, extent[axis_at] // shards_of).reshape([-1 if axis == axis_at else 1 for axis in range(len(extent))])
    return level


def choose_distinct(stream_key, rows, number_of, top, lift):
    order = jax.random.permutation(jax.random.fold_in(stream_key, 1), number_of)
    pull = order
    for power in range(3):
        pull = pull * pull // number_of
    pull = pull * lift // number_of
    tickets = jax.random.randint(jax.random.fold_in(stream_key, 2), (rows, number_of), 0, 4096) + pull
    holders = jax.random.permutation(jax.random.fold_in(stream_key, 3), rows)[jnp.arange(number_of) % rows]
    tickets = jnp.where(jnp.arange(rows)[:, None] == holders[None, :], 1 << 14, tickets)
    score = tickets * number_of + jnp.arange(number_of)
    return lax.top_k(score.astype(jnp.int32), top)[1].astype(jnp.int32)


def scatter_about(rng, extent, width, bound, pieces=(), kind=jnp.bfloat16):
    loudness = levels(rng, extent, pieces, -0.22, 0.18) if pieces else 1.0
    values = jax.random.normal(rng, extent, jnp.float32) * width * loudness
    return jnp.minimum(jnp.maximum(values, -bound), bound).astype(kind)


def setup_inputs(seed: int = 0) -> dict:
    key_list = jax.random.split(jax.random.key(seed), 19)
    images = scatter_about(key_list[0], (IMAGES, LENGTH, D), 1.0, 6.0, ((0, 8), (1, 4)))
    cotangent = scatter_about(key_list[1], (IMAGES, LENGTH, D), 1.0, 6.0, ((0, 8), (1, 4)))
    key_mask = draw_key_mask(jax.random.fold_in(key_list[18], 71), 0)
    routes = choose_distinct(key_list[3], IMAGES * LENGTH, EXPERTS, 2, 4096).reshape((IMAGES, LENGTH, 2))
    fill_order = draw_fill_order(jax.random.fold_in(key_list[18], 71), 0)
    norm_gain1 = jnp.clip(1.0 + 0.18 * jax.random.normal(key_list[5], (D,), jnp.float32), 0.099609375, 1.8984375).astype(jnp.bfloat16)
    qkv_weight1 = scatter_about(key_list[6], (D, 3 * D), D ** -0.5, 0.21875, ((0, 8),))
    proj_weight1 = scatter_about(key_list[7], (D, D), (max(1, 2 * D // LENGTH)) ** -0.5, 6.0, ((0, 8),))
    norm_gain2 = jnp.clip(1.0 + 0.18 * jax.random.normal(key_list[8], (D,), jnp.float32), 0.099609375, 1.8984375).astype(jnp.bfloat16)
    fc_in = scatter_about(key_list[9], (D, FF), D ** -0.5, 0.21875, ((0, 8),))
    fc_out = scatter_about(key_list[10], (FF, D), FF ** -0.5, 0.109375, ((0, 8),))
    norm_gain3 = jnp.clip(1.0 + 0.18 * jax.random.normal(key_list[11], (D,), jnp.float32), 0.099609375, 1.8984375).astype(jnp.bfloat16)
    qkv_weight2 = scatter_about(key_list[12], (D, 3 * D), D ** -0.5, 0.21875, ((0, 8),))
    proj_weight2 = scatter_about(key_list[13], (D, D), (max(1, 2 * D // LENGTH)) ** -0.5, 6.0, ((0, 8),))
    norm_gain4 = jnp.clip(1.0 + 0.18 * jax.random.normal(key_list[14], (D,), jnp.float32), 0.099609375, 1.8984375).astype(jnp.bfloat16)
    router = scatter_about(key_list[15], (D, EXPERTS), D ** -0.5, 0.21875, ((0, 8),))
    expert_in = scatter_about(key_list[16], (2 * EXPERTS, D, FE // 2), D ** -0.5, 0.21875, ((0, 8),))
    expert_out = scatter_about(key_list[17], (2 * EXPERTS, FE // 2, D), (max(1, FE // 1024)) ** -0.5, 3.5, ((0, 8),))
    return dict(images=images, cotangent=cotangent, key_mask=key_mask, routes=routes, fill_order=fill_order, norm_gain1=norm_gain1, qkv_weight1=qkv_weight1, proj_weight1=proj_weight1, norm_gain2=norm_gain2, fc_in=fc_in, fc_out=fc_out, norm_gain3=norm_gain3, qkv_weight2=qkv_weight2, proj_weight2=proj_weight2, norm_gain4=norm_gain4, router=router, expert_in=expert_in, expert_out=expert_out)


HIGHEST = lax.Precision.HIGHEST

@jax.custom_vjp
def low(v):
    return lax.optimization_barrier(v.astype(jnp.bfloat16)).astype(jnp.float32)

@jax.custom_vjp
def low_back(v):
    return v

def low_keep(v):
    return (low(v), None)

def low_pass(kept, grad):
    return (grad,)

def back_keep(v):
    return (v, None)

def back_low(kept, grad):
    return (low(grad),)
low.defvjp(low_keep, low_pass)
low_back.defvjp(back_keep, back_low)

def layer_norm(values, gain):
    centred = values - lax.optimization_barrier(jnp.mean(values, axis=-1, keepdims=True))
    variance = lax.optimization_barrier(jnp.mean(centred * centred, axis=-1, keepdims=True))
    return centred * lax.rsqrt(variance + 1e-06) * gain

def gelu_exact(values):
    return jax.nn.gelu(values, approximate=False)

def attention(residual, gain, qkv_weight, proj_weight, valid):
    normed_low = low(layer_norm(residual, gain))
    packed = low(low_back(jnp.dot(normed_low, qkv_weight, precision=HIGHEST)))
    heads = packed.reshape(LENGTH, 3, HEADS, HEAD_DIM)
    raw_scores = jnp.einsum('qhd,khd->hqk', heads[:, 0], heads[:, 1], precision=HIGHEST)
    scores = jnp.where(valid[None, None, :], low_back(raw_scores) * HEAD_DIM ** (-0.5), -1e+30)
    attn_probs = jax.nn.softmax(scores, axis=-1)
    mixed = low(low_back(jnp.einsum('hqk,khd->qhd', low(attn_probs), heads[:, 2], precision=HIGHEST)))
    return low_back(jnp.dot(mixed.reshape(LENGTH, D), proj_weight, precision=HIGHEST))

def feed_forward(residual, gain, weight_in, weight_out):
    normed_low = low(layer_norm(residual, gain))
    pre_act = low_back(jnp.dot(normed_low, weight_in, precision=HIGHEST))
    hidden = low(gelu_exact(pre_act))
    return low_back(jnp.dot(hidden, weight_out, precision=HIGHEST))

def destinations(route, order):

    def one_block(route_block, order_block):
        pair_expert = route_block.reshape(-1)
        pair_key = (jnp.arange(2, dtype=jnp.int32)[None, :] * TOK_DEV + order_block[:, None]).reshape(-1)
        same_expert = pair_expert[:, None] == pair_expert[None, :]
        earlier = pair_key[None, :] < pair_key[:, None]
        slot_rank = lax.optimization_barrier(jnp.sum((same_expert & earlier).astype(jnp.int32), axis=1))
        return (pair_expert, slot_rank)
    pair_expert, slot_rank = jax.vmap(one_block)(route.reshape(N_SEQ, TOK_DEV, 2), order.reshape(N_SEQ, TOK_DEV))
    source = jnp.arange(N_SEQ, dtype=jnp.int32)[:, None]
    target = jnp.where(slot_rank < CAPACITY, pair_expert * (N_SEQ * CAPACITY) + source * CAPACITY + slot_rank, EXPERTS * N_SEQ * CAPACITY).reshape(-1).astype(jnp.int32)
    slot_pair = jnp.full((EXPERTS * N_SEQ * CAPACITY + 1,), 2 * LENGTH, jnp.int32)
    slot_pair = slot_pair.at[target].set(jnp.arange(2 * LENGTH, dtype=jnp.int32))
    return (target, slot_pair[:-1])

def mixture(residual, gain, router, expert_in, expert_out, route, order):
    normed_low = low(layer_norm(residual, gain))
    logits = low_back(jnp.dot(normed_low, router, precision=HIGHEST))
    router_probs = jax.nn.softmax(logits, axis=-1)
    gates = jnp.take_along_axis(router_probs, route, axis=1)
    target, slot_pair = destinations(route, order)
    pair_rows = jnp.concatenate([jnp.repeat(normed_low, 2, axis=0), jnp.zeros((1, D), jnp.float32)], axis=0)
    batch = pair_rows[slot_pair].reshape(EXPERTS, N_SEQ * CAPACITY, D)
    in_halves = expert_in.reshape(EXPERTS, 2, D, FE // 2)
    out_halves = expert_out.reshape(EXPERTS, 2, FE // 2, D)
    summed = jnp.zeros_like(batch)
    for half in range(2):
        inputs = low_back(batch)
        pre_act = low_back(jnp.einsum('erd,edf->erf', inputs, in_halves[:, half], precision=HIGHEST))
        hidden = low(gelu_exact(pre_act))
        summed = summed + low_back(low(jnp.einsum('erf,efd->erd', hidden, out_halves[:, half], precision=HIGHEST)))
    flat_rows = jnp.concatenate([summed.reshape(-1, D), jnp.zeros((1, D), jnp.float32)], axis=0)
    picked = flat_rows[target].reshape(LENGTH, 2, D)
    return lax.optimization_barrier(jnp.sum(gates[:, :, None] * picked, axis=1))

def image_forward(params, start, valid, route, order):
    gain_one, qkv_one, proj_one, gain_two, weight_in, weight_out, gain_three, qkv_two, proj_two, gain_four, router, expert_in, expert_out = params
    first = start + attention(start, gain_one, qkv_one, proj_one, valid)
    second = first + feed_forward(first, gain_two, weight_in, weight_out)
    third = second + attention(second, gain_three, qkv_two, proj_two, valid)
    return third + mixture(third, gain_four, router, expert_in, expert_out, route, order)

def reference(images, cotangent, key_mask, routes, fill_order, norm_gain1, qkv_weight1, proj_weight1, norm_gain2, fc_in, fc_out, norm_gain3, qkv_weight2, proj_weight2, norm_gain4, router, expert_in, expert_out):
    weights = (norm_gain1.astype(jnp.float32), qkv_weight1.astype(jnp.float32), proj_weight1.astype(jnp.float32), norm_gain2.astype(jnp.float32), fc_in.astype(jnp.float32), fc_out.astype(jnp.float32), norm_gain3.astype(jnp.float32), qkv_weight2.astype(jnp.float32), proj_weight2.astype(jnp.float32), norm_gain4.astype(jnp.float32), router.astype(jnp.float32), expert_in.astype(jnp.float32), expert_out.astype(jnp.float32))

    def one_image(totals, inputs):
        image, grad_out, mask_row, route, order = inputs
        valid = mask_row > 0

        def forward(params, start):
            return image_forward(params, start, valid, route, order)
        result, pullback = jax.vjp(forward, weights, image.astype(jnp.float32))
        grads, image_grad = pullback(grad_out.astype(jnp.float32))
        return (jax.tree.map(jnp.add, totals, grads), (result, image_grad))
    zeros = jax.tree.map(jnp.zeros_like, weights)
    totals, (outputs, image_grads) = lax.scan(one_image, zeros, (images, cotangent, key_mask, routes, fill_order))
    return (outputs, image_grads, totals[0], totals[1], totals[2], totals[3], totals[4], totals[5], totals[6], totals[7], totals[8], totals[9], totals[10], totals[11], totals[12])
```

```python
import functools

import jax
import jax.numpy as jnp
from jax import lax
from jax.experimental import pallas as pl
from jax.experimental.pallas import tpu as pltpu
from jax.sharding import PartitionSpec as P

HEAD_DIM = 64
LANES = 128
ROW_TILE = 16
F32 = jnp.float32
BF16 = jnp.bfloat16
VMEM = pl.BlockSpec(memory_space=pltpu.VMEM)
NT = (((1,), (1,)), ((), ()))


def round_up(n, m):
    return -(-n // m) * m


def seq_places():
    me = lax.axis_index("seq")
    near = me + 1 - 2 * lax.rem(me, 2)
    across = lax.rem(me + 2, 4)
    far = lax.rem(near + 2, 4)
    return me, near, across, far


def cuts_of(rows, parts):
    tiles = rows // ROW_TILE
    edges = [(tiles * i // parts) * ROW_TILE for i in range(parts + 1)]
    return [(a, b - a) for a, b in zip(edges[:-1], edges[1:])]


def remote(src, dst, sems, n, axis, place):
    return pltpu.make_async_remote_copy(
        src_ref=src,
        dst_ref=dst,
        send_sem=sems.at[0, n],
        recv_sem=sems.at[1, n],
        device_id={axis: place},
        device_id_type=pl.DeviceIdType.MESH,
    )


def greet(seq_peers, wide_peers=()):
    barrier = pltpu.get_barrier_semaphore()
    for place in seq_peers:
        pl.semaphore_signal(
            barrier, inc=1, device_id={"seq": place}, device_id_type=pl.DeviceIdType.MESH
        )
    for place in wide_peers:
        pl.semaphore_signal(
            barrier, inc=1, device_id={"wide": place}, device_id_type=pl.DeviceIdType.MESH
        )
    pl.semaphore_wait(barrier, len(seq_peers) + len(wide_peers))


class RowScatter:
    def __init__(self, partial, got, sent, crossed, sems, cuts):
        self.partial, self.got, self.sent, self.crossed = partial, got, sent, crossed
        me, near, across, far = seq_places()
        self.me, self.across = me, across
        self.cuts = cuts
        self.far_part, self.near_part, self.cross = [], [], []
        for i, (at, size) in enumerate(cuts):
            rows = pl.ds(at, size)
            self.far_part.append(
                remote(partial.at[far, rows], got.at[1, rows], sems, 3 * i, "seq", near)
            )
            self.near_part.append(
                remote(partial.at[near, rows], got.at[0, rows], sems, 3 * i + 1, "seq", near)
            )
            self.cross.append(
                remote(sent.at[rows], crossed.at[rows], sems, 3 * i + 2, "seq", across)
            )

    def start(self):
        for copy in self.far_part:
            copy.start()
        for copy in self.near_part:
            copy.start()
        for i, (at, size) in enumerate(self.cuts):
            rows = pl.ds(at, size)
            self.far_part[i].wait_recv()
            self.sent[rows, :] = (
                self.partial[self.across, rows].astype(F32) + self.got[1, rows].astype(F32)
            ).astype(BF16)
            self.cross[i].start()

    def total(self, i):
        at, size = self.cuts[i]
        rows = pl.ds(at, size)
        self.near_part[i].wait_recv()
        chip = self.partial[self.me, rows].astype(F32) + self.got[0, rows].astype(F32)
        self.cross[i].wait_recv()
        return chip + self.crossed[rows, :].astype(F32)

    def finish(self):
        for copy in self.far_part + self.near_part + self.cross:
            copy.wait_send()


class RowGather:
    def __init__(self, whole, sems, cuts):
        self.whole = whole
        me, near, across, far = seq_places()
        self.me = me
        self.cuts = cuts
        self.near_copy, self.cross, self.onward = [], [], []
        for i, (at, size) in enumerate(cuts):
            mine = whole.at[me, pl.ds(at, size)]
            theirs = whole.at[across, pl.ds(at, size)]
            self.near_copy.append(remote(mine, mine, sems, 3 * i, "seq", near))
            self.cross.append(remote(mine, mine, sems, 3 * i + 1, "seq", across))
            self.onward.append(remote(theirs, theirs, sems, 3 * i + 2, "seq", near))

    def send(self, i, rows):
        at, size = self.cuts[i]
        self.whole[self.me, pl.ds(at, size)] = rows
        self.cross[i].start()
        self.near_copy[i].start()

    def finish(self):
        for i in range(len(self.cuts)):
            self.cross[i].wait_recv()
            self.onward[i].start()
        for copy in self.near_copy + self.onward:
            copy.wait_recv()
        for copy in self.near_copy + self.cross + self.onward:
            copy.wait_send()


def real_rows(at, size, tokens):
    return at + lax.broadcasted_iota(jnp.int32, (size, 1), 0) < tokens


def centre(values):
    centred = values - jnp.mean(values, axis=-1, keepdims=True)
    variance = jnp.mean(centred * centred, axis=-1, keepdims=True)
    scale = lax.rsqrt(variance + 1e-06)
    return centred * scale, scale


def norm_forward(values, gain):
    return centre(values)[0] * gain


def norm_backward(values, gain, grad):
    unit, scale = centre(values)
    grad_unit = grad * gain
    grad_in = scale * (
        grad_unit
        - jnp.mean(grad_unit, axis=-1, keepdims=True)
        - unit * jnp.mean(grad_unit * unit, axis=-1, keepdims=True)
    )
    return grad_in, jnp.sum(grad * unit, axis=0, keepdims=True)


def sems(n):
    return pltpu.SemaphoreType.DMA((2, n))


def scatter_scratch(rows, width, parts):
    return [
        pltpu.VMEM((2, rows, width), BF16),
        pltpu.VMEM((rows, width), BF16),
        pltpu.VMEM((rows, width), BF16),
        sems(3 * parts),
    ]


def comm_params(collective_id):
    return pltpu.CompilerParams(collective_id=collective_id, has_side_effects=True)


PARTS = 2


def spread_norm(residual, gain, tokens, collective_id):
    rows, width = residual.shape
    cuts = cuts_of(rows, PARTS)

    def kernel(residual_ref, gain_ref, whole_ref, gather_sems):
        _, near, across, _ = seq_places()
        gather = RowGather(whole_ref, gather_sems, cuts)
        greet((near, across))
        for i, (at, size) in enumerate(cuts):
            normed = norm_forward(residual_ref[pl.ds(at, size), :], gain_ref[...])
            normed = jnp.where(real_rows(at, size, tokens), normed, 0.0)
            gather.send(i, normed.astype(BF16))
        gather.finish()

    return pl.pallas_call(
        kernel,
        out_shape=jax.ShapeDtypeStruct((4, rows, width), BF16),
        in_specs=[VMEM] * 2,
        out_specs=VMEM,
        scratch_shapes=[sems(3 * PARTS)],
        compiler_params=comm_params(collective_id),
    )(residual, gain)


def join_forward(partial, residual, gain, tokens, collective_id):
    rows, width = residual.shape
    cuts = cuts_of(rows, PARTS)

    def kernel(
        partial_ref, residual_ref, gain_ref, out_ref, whole_ref, got, sent, crossed, s_sems, g_sems
    ):
        _, near, across, _ = seq_places()
        scatter = RowScatter(partial_ref, got, sent, crossed, s_sems, cuts)
        gather = RowGather(whole_ref, g_sems, cuts)
        greet((near, across))
        scatter.start()
        for i, (at, size) in enumerate(cuts):
            total = residual_ref[pl.ds(at, size), :] + scatter.total(i)
            out_ref[pl.ds(at, size), :] = total
            normed = norm_forward(total, gain_ref[...])
            normed = jnp.where(real_rows(at, size, tokens), normed, 0.0)
            gather.send(i, normed.astype(BF16))
        gather.finish()
        scatter.finish()

    return pl.pallas_call(
        kernel,
        out_shape=(
            jax.ShapeDtypeStruct((rows, width), F32),
            jax.ShapeDtypeStruct((4, rows, width), BF16),
        ),
        in_specs=[VMEM] * 3,
        out_specs=(VMEM, VMEM),
        scratch_shapes=scatter_scratch(rows, width, PARTS) + [sems(3 * PARTS)],
        compiler_params=comm_params(collective_id),
    )(partial, residual, gain)


def join_backward(partial, residual, gain, grad, tokens, collective_id, last):
    rows, width = residual.shape
    cuts = cuts_of(rows, PARTS)

    def kernel(partial_ref, residual_ref, gain_ref, grad_ref, out_ref, gain_grad_ref, *rest):
        if last:
            got, sent, crossed, s_sems = rest
        else:
            whole_ref, got, sent, crossed, s_sems, g_sems = rest
            gather = RowGather(whole_ref, g_sems, cuts)
        _, near, across, _ = seq_places()
        scatter = RowScatter(partial_ref, got, sent, crossed, s_sems, cuts)
        greet((near, across))
        scatter.start()
        gain_grad = jnp.zeros((1, width), F32)
        for i, (at, size) in enumerate(cuts):
            rows_here = pl.ds(at, size)
            grad_in, term = norm_backward(
                residual_ref[rows_here, :], gain_ref[...], scatter.total(i)
            )
            gain_grad = gain_grad + term
            grad_out = grad_ref[rows_here, :] + grad_in
            if last:
                keep = min(size, tokens - at)
                out_ref[pl.ds(at, keep), :] = grad_out[:keep]
            else:
                out_ref[rows_here, :] = grad_out
                gather.send(i, grad_out.astype(BF16))
        gain_grad_ref[...] = gain_grad
        if not last:
            gather.finish()
        scatter.finish()

    out_shape = [
        jax.ShapeDtypeStruct((tokens if last else rows, width), F32),
        jax.ShapeDtypeStruct((1, width), F32),
    ]
    scratch = scatter_scratch(rows, width, PARTS)
    if not last:
        out_shape.append(jax.ShapeDtypeStruct((4, rows, width), BF16))
        scratch.append(sems(3 * PARTS))
    return pl.pallas_call(
        kernel,
        out_shape=tuple(out_shape),
        in_specs=[VMEM] * 4,
        out_specs=(VMEM,) * len(out_shape),
        scratch_shapes=scratch,
        compiler_params=comm_params(collective_id),
    )(partial, residual, gain, grad)


def head_lanes(rows, head):
    lane = lax.broadcasted_iota(jnp.int32, (rows, LANES), 1)
    low = (head % 2) * HEAD_DIM
    return (lane >= low) & (lane < low + HEAD_DIM)


def attend_forward(normed_all, wqkv, wproj, bias_row, heads):
    blocks, rows, width = normed_all.shape
    group = wproj.shape[0]
    total = blocks * rows

    def kernel(normed_ref, wqkv_ref, wproj_ref, bias_ref, qkv_ref, lse_ref, mixed_ref, part_ref):
        step = pl.program_id(0)

        @pl.when(step == 0)
        def _():
            @pl.loop(0, blocks)
            def _(b):
                qkv_ref[b] = jnp.dot(
                    normed_ref[b], wqkv_ref[...], preferred_element_type=F32
                ).astype(BF16)

        lane = lax.broadcasted_iota(jnp.int32, (rows, LANES), 1)
        lse = jnp.zeros((rows, LANES), F32)
        for pair in range(group // LANES):
            lo = pair * LANES
            query = qkv_ref[step, :, lo : lo + LANES].astype(F32) * HEAD_DIM ** (-0.5)
            keys = qkv_ref[:, :, group + lo : group + lo + LANES].reshape(total, LANES)
            values = qkv_ref[:, :, 2 * group + lo : 2 * group + lo + LANES].reshape(total, LANES)
            mixed = jnp.zeros((rows, LANES), F32)
            for head in range(2 * pair, min(2 * pair + 2, heads)):
                mine = head_lanes(rows, head)
                scores = lax.dot_general(
                    jnp.where(mine, query, 0.0).astype(BF16), keys, NT, preferred_element_type=F32
                )
                scores = scores + bias_ref[...]
                peak = jnp.max(scores, axis=-1, keepdims=True)
                exps = jnp.exp(scores - peak)
                row_total = jnp.sum(exps, axis=-1, keepdims=True)
                out = jnp.dot(exps.astype(BF16), values, preferred_element_type=F32)
                mixed = jnp.where(mine, out / row_total, mixed)
                lse = jnp.where(lane == head, peak + jnp.log(row_total), lse)
            mixed_ref[step, :, lo : lo + LANES] = mixed.astype(BF16)
        lse_ref[step] = lse
        part_ref[step] = jnp.dot(
            mixed_ref[step], wproj_ref[...], preferred_element_type=F32
        ).astype(BF16)

    def whole(*shape):
        return pl.BlockSpec(shape, lambda i: (0,) * len(shape))

    return pl.pallas_call(
        kernel,
        grid=(blocks,),
        out_shape=(
            jax.ShapeDtypeStruct((blocks, rows, 3 * group), BF16),
            jax.ShapeDtypeStruct((blocks, rows, LANES), F32),
            jax.ShapeDtypeStruct((blocks, rows, group), BF16),
            jax.ShapeDtypeStruct((blocks, rows, width), BF16),
        ),
        in_specs=[
            whole(blocks, rows, width),
            whole(width, 3 * group),
            whole(group, width),
            whole(1, total),
        ],
        out_specs=(
            whole(blocks, rows, 3 * group),
            whole(blocks, rows, LANES),
            whole(blocks, rows, group),
            whole(blocks, rows, width),
        ),
        compiler_params=pltpu.CompilerParams(dimension_semantics=("arbitrary",)),
    )(normed_all, wqkv, wproj, bias_row)


def attend_backward(branch_all, qkv, lse, mixed, wqkv, wproj, bias_col, heads):
    blocks, rows, width = branch_all.shape
    group = wproj.shape[0]
    pairs = group // LANES
    total = blocks * rows

    def kernel(
        branch_ref,
        qkv_ref,
        lse_ref,
        mixed_ref,
        wqkv_ref,
        wproj_ref,
        bias_ref,
        grad_ref,
        part_ref,
        gm_ref,
        query_ref,
        grads_ref,
        stats_ref,
        dq_ref,
    ):
        step = pl.program_id(0)

        @pl.when(step == 0)
        def _():
            @pl.loop(0, blocks)
            def _(b):
                gm_ref[b] = lax.dot_general(
                    branch_ref[b], wproj_ref[...], NT, preferred_element_type=F32
                ).astype(BF16)

            lse_rows = lse_ref[...].reshape(total, LANES).T
            for head in range(heads):
                lo = (head // 2) * LANES
                mine = head_lanes(total, head)
                query = qkv_ref[:, :, lo : lo + LANES].reshape(total, LANES).astype(F32)
                query_ref[head] = jnp.where(mine, query * HEAD_DIM ** (-0.5), 0.0).astype(BF16)
                grads = gm_ref[:, :, lo : lo + LANES].reshape(total, LANES).astype(F32)
                grads = jnp.where(mine, grads, 0.0)
                grads_ref[head] = grads.astype(BF16)
                out = mixed_ref[:, :, lo : lo + LANES].reshape(total, LANES).astype(F32)
                stats_ref[head] = jnp.concatenate(
                    [
                        lse_rows[head : head + 1],
                        jnp.sum((grads * out).T, axis=0, keepdims=True),
                        jnp.zeros((6, total), F32),
                    ],
                    axis=0,
                )
            dq_ref[...] = jnp.zeros_like(dq_ref)

        for pair in range(pairs):
            lo = pair * LANES
            keys = qkv_ref[step, :, group + lo : group + lo + LANES]
            values = qkv_ref[step, :, 2 * group + lo : 2 * group + lo + LANES]
            grad_keys = jnp.zeros((rows, LANES), F32)
            grad_values = jnp.zeros((rows, LANES), F32)
            for head in range(2 * pair, min(2 * pair + 2, heads)):
                scores = lax.dot_general(keys, query_ref[head], NT, preferred_element_type=F32)
                probs = jnp.exp(scores + bias_ref[step] - stats_ref[head, 0:1])
                grad_probs = lax.dot_general(
                    values, grads_ref[head], NT, preferred_element_type=F32
                )
                grad_scores = (probs * (grad_probs - stats_ref[head, 1:2])).astype(BF16)
                grad_values += jnp.dot(
                    probs.astype(BF16), grads_ref[head], preferred_element_type=F32
                )
                grad_keys += jnp.dot(grad_scores, query_ref[head], preferred_element_type=F32)
                mine = head_lanes(rows, head)
                own_keys = jnp.where(mine, keys.astype(F32), 0.0).T.astype(BF16)
                dq_ref[pl.ds(lo, LANES), :] += jnp.dot(
                    own_keys, grad_scores, preferred_element_type=F32
                )
            grad_ref[step, :, group + lo : group + lo + LANES] = grad_keys.astype(BF16)
            grad_ref[step, :, 2 * group + lo : 2 * group + lo + LANES] = grad_values.astype(BF16)

        @pl.when(step == blocks - 1)
        def _():
            for pair in range(pairs):
                lo = pair * LANES
                grad_query = dq_ref[pl.ds(lo, LANES), :].T * HEAD_DIM ** (-0.5)
                grad_ref[:, :, lo : lo + LANES] = grad_query.astype(BF16).reshape(
                    blocks, rows, LANES
                )

            @pl.loop(0, blocks)
            def _(b):
                part_ref[b] = lax.dot_general(
                    grad_ref[b], wqkv_ref[...], NT, preferred_element_type=F32
                ).astype(BF16)

    def whole(*shape):
        return pl.BlockSpec(shape, lambda i: (0,) * len(shape))

    return pl.pallas_call(
        kernel,
        grid=(blocks,),
        out_shape=(
            jax.ShapeDtypeStruct((blocks, rows, 3 * group), BF16),
            jax.ShapeDtypeStruct((blocks, rows, width), BF16),
        ),
        in_specs=[
            whole(blocks, rows, width),
            whole(blocks, rows, 3 * group),
            whole(blocks, rows, LANES),
            whole(blocks, rows, group),
            whole(width, 3 * group),
            whole(group, width),
            whole(blocks, rows, 1),
        ],
        out_specs=(whole(blocks, rows, 3 * group), whole(blocks, rows, width)),
        scratch_shapes=[
            pltpu.VMEM((blocks, rows, group), BF16),
            pltpu.VMEM((heads, total, LANES), BF16),
            pltpu.VMEM((heads, total, LANES), BF16),
            pltpu.VMEM((heads, 8, total), F32),
            pltpu.VMEM((group, total), F32),
        ],
        compiler_params=pltpu.CompilerParams(dimension_semantics=("arbitrary",)),
    )(branch_all, qkv, lse, mixed, wqkv, wproj, bias_col)


def wide_places():
    me = lax.axis_index("wide")
    half = lax.rem(me, 2)
    return me, half, me // 2, me + 1 - 2 * half


def dispatch(partial, residual, gain, router, routes, cotangent, target, tokens, slots, cid):
    rows, width = residual.shape
    wide = lax.axis_size("wide")
    experts = wide // 2
    cuts = cuts_of(rows, PARTS)

    def kernel(
        partial_ref,
        residual_ref,
        gain_ref,
        router_ref,
        routes_ref,
        cot_ref,
        target_ref,
        third_ref,
        routed_ref,
        probs_ref,
        gates_ref,
        rows_ref,
        grads_ref,
        got,
        sent,
        crossed,
        s_sems,
        send_rows,
        send_grads,
        gated_ref,
        e_sems,
        p_sems,
    ):
        _, near, across, _ = seq_places()
        me, half, expert, partner = wide_places()
        scatter = RowScatter(partial_ref, got, sent, crossed, s_sems, cuts)
        others = [lax.rem(expert + d, experts) for d in range(1, experts)]
        greet((near, across), [2 * e + half for e in others] + [partner])
        scatter.start()
        for i, (at, size) in enumerate(cuts):
            here = pl.ds(at, size)
            total = residual_ref[here, :] + scatter.total(i)
            third_ref[here, :] = total
            normed = norm_forward(total, gain_ref[...])
            normed = jnp.where(real_rows(at, size, tokens), normed, 0.0)
            routed_ref[here, :] = normed.astype(BF16)
        scatter.finish()

        slot = lax.broadcasted_iota(jnp.int32, (slots, rows), 0)

        def chosen(e, k):
            return (slot + e * slots == target_ref[k : k + 1, :]).astype(F32)

        def exchange(block_of, send, out, base):
            first = []
            for d, e in enumerate(others):
                send[d] = block_of(e)
                first.append(
                    remote(send.at[d], out.at[me], e_sems, base + d, "wide", 2 * e + half)
                )
                first[-1].start()
            out[me] = block_of(expert)
            return first

        def pass_on(first, out, base):
            second = [remote(out.at[me], out.at[me], p_sems, base, "wide", partner)]
            second[0].start()
            for d in range(1, experts):
                first[d - 1].wait_recv()
                source = 2 * lax.rem(expert + experts - d, experts) + half
                second.append(
                    remote(out.at[source], out.at[source], p_sems, base + d, "wide", partner)
                )
                second[-1].start()
            return second

        def row_block(e):
            pick = (chosen(e, 0) + chosen(e, 1)).astype(BF16)
            return jnp.dot(pick, routed_ref[...], preferred_element_type=F32).astype(BF16)

        first_rows = exchange(row_block, send_rows, rows_ref, 0)

        lane = lax.broadcasted_iota(jnp.int32, (rows, LANES), 1)
        logits = jnp.dot(routed_ref[...], router_ref[...], preferred_element_type=F32)
        logits = jnp.where(lane < experts, logits, -1e30)
        exps = jnp.exp(logits - jnp.max(logits, axis=-1, keepdims=True))
        probs = exps / jnp.sum(exps, axis=-1, keepdims=True)
        probs_ref[...] = probs
        gates = jnp.zeros((rows, LANES), F32)
        for k in range(2):
            gate = jnp.sum(
                jnp.where(lane == routes_ref[:, k : k + 1], probs, 0.0), axis=-1, keepdims=True
            )
            gates = jnp.where(lane == k, gate, gates)
            gated_ref[k] = (gate * cot_ref[...].astype(F32)).astype(BF16)
        gates_ref[...] = gates

        def grad_block(e):
            both = jnp.dot(chosen(e, 0).astype(BF16), gated_ref[0], preferred_element_type=F32)
            both += jnp.dot(chosen(e, 1).astype(BF16), gated_ref[1], preferred_element_type=F32)
            return both.astype(BF16)

        first_grads = exchange(grad_block, send_grads, grads_ref, experts)
        second = pass_on(first_rows, rows_ref, 0)
        second += pass_on(first_grads, grads_ref, experts)
        for copy in second:
            copy.wait_recv()
        for copy in first_rows + first_grads + second:
            copy.wait_send()

    return pl.pallas_call(
        kernel,
        out_shape=(
            jax.ShapeDtypeStruct((rows, width), F32),
            jax.ShapeDtypeStruct((rows, width), BF16),
            jax.ShapeDtypeStruct((rows, LANES), F32),
            jax.ShapeDtypeStruct((rows, LANES), F32),
            jax.ShapeDtypeStruct((wide, slots, width), BF16),
            jax.ShapeDtypeStruct((wide, slots, width), BF16),
        ),
        in_specs=[VMEM] * 7,
        out_specs=(VMEM,) * 6,
        scratch_shapes=scatter_scratch(rows, width, PARTS)
        + [
            pltpu.VMEM((experts - 1, slots, width), BF16),
            pltpu.VMEM((experts - 1, slots, width), BF16),
            pltpu.VMEM((2, rows, width), BF16),
            sems(2 * experts),
            sems(2 * experts),
        ],
        compiler_params=comm_params(cid),
    )(partial, residual, gain, router, routes, cotangent, target)


def combine(
    part, row_grads, third, routed, probs, gates, gain, router, routes, cotangent, target, tokens, cid
):
    wide, slots, width = part.shape
    experts = wide // 2
    rows = third.shape[0]
    cuts = cuts_of(rows, PARTS)

    def kernel(
        part_ref,
        row_grads_ref,
        third_ref,
        routed_ref,
        probs_ref,
        gates_ref,
        gain_ref,
        router_ref,
        routes_ref,
        cot_ref,
        target_ref,
        output_ref,
        grad_ref,
        gain_grad_ref,
        router_grad_ref,
        whole_ref,
        from_part,
        from_grads,
        send_part,
        send_grads,
        back_part,
        back_grads,
        e_sems,
        p_sems,
        g_sems,
    ):
        _, near, across, _ = seq_places()
        me, half, expert, partner = wide_places()
        gather = RowGather(whole_ref, g_sems, cuts)
        homes = [lax.rem(expert + d, experts) for d in range(1, experts)] + [expert]
        greet((near, across), [2 * h + half for h in homes[:-1]] + [partner])

        def halves(src, into, base):
            copies = []
            for d, home in enumerate(homes):
                copies.append(
                    remote(
                        src.at[2 * home + 1 - half], into.at[d], p_sems, base + d, "wide", partner
                    )
                )
                copies[-1].start()
            return copies

        def homeward(copies, src, arrived, send, back, base):
            sent = []
            for d, home in enumerate(homes):
                copies[d].wait_recv()
                both = (src[2 * home + half].astype(F32) + arrived[d].astype(F32)).astype(BF16)
                if d == experts - 1:
                    back[expert] = both
                else:
                    send[d] = both
                    sent.append(
                        remote(
                            send.at[d], back.at[expert], e_sems, base + d, "wide", 2 * home + half
                        )
                    )
                    sent[-1].start()
            return sent

        part_halves = halves(part_ref, from_part, 0)
        grad_halves = halves(row_grads_ref, from_grads, experts)
        part_sent = homeward(part_halves, part_ref, from_part, send_part, back_part, 0)
        grad_sent = homeward(
            grad_halves, row_grads_ref, from_grads, send_grads, back_grads, experts
        )

        spot = lax.broadcasted_iota(jnp.int32, (rows, experts * slots), 1)
        picks = [(spot == target_ref[:, k : k + 1]).astype(F32) for k in range(2)]
        cot = cot_ref[...].astype(F32)
        lane = lax.broadcasted_iota(jnp.int32, (rows, LANES), 1)
        for copy in part_sent:
            copy.wait_recv()
        returned = back_part[...].reshape(experts * slots, width)
        output = third_ref[...]
        grad_probs = jnp.zeros((rows, LANES), F32)
        for k in range(2):
            picked = jnp.dot(picks[k].astype(BF16), returned, preferred_element_type=F32)
            output += gates_ref[:, k : k + 1] * picked
            grad_gate = jnp.sum(cot * picked, axis=-1, keepdims=True)
            grad_probs += jnp.where(lane == routes_ref[:, k : k + 1], grad_gate, 0.0)
        output_ref[...] = output[:tokens]
        probs = probs_ref[...]
        delta = jnp.sum(probs * grad_probs, axis=-1, keepdims=True)
        logit_grad = probs * (grad_probs - delta)
        logit_low = logit_grad.astype(BF16)
        router_grad_ref[...] = jnp.dot(
            logit_low.astype(F32).T.astype(BF16), routed_ref[...], preferred_element_type=F32
        )
        routed_grad = lax.dot_general(
            logit_low, router_ref[...], NT, preferred_element_type=F32
        )
        for copy in grad_sent:
            copy.wait_recv()
        routed_grad += jnp.dot(
            (picks[0] + picks[1]).astype(BF16),
            back_grads[...].reshape(experts * slots, width),
            preferred_element_type=F32,
        )
        grad_in, gain_grad = norm_backward(third_ref[...], gain_ref[...], routed_grad)
        gain_grad_ref[...] = gain_grad
        grad_ref[...] = cot + grad_in
        for i, (at, size) in enumerate(cuts):
            gather.send(i, grad_ref[pl.ds(at, size), :].astype(BF16))
        gather.finish()
        for copy in part_halves + grad_halves + part_sent + grad_sent:
            copy.wait_send()

    blocks = pltpu.VMEM((experts, slots, width), BF16)
    sends = pltpu.VMEM((experts - 1, slots, width), BF16)
    return pl.pallas_call(
        kernel,
        out_shape=(
            jax.ShapeDtypeStruct((tokens, width), F32),
            jax.ShapeDtypeStruct((rows, width), F32),
            jax.ShapeDtypeStruct((1, width), F32),
            jax.ShapeDtypeStruct((LANES, width), F32),
            jax.ShapeDtypeStruct((4, rows, width), BF16),
        ),
        in_specs=[VMEM] * 11,
        out_specs=(VMEM,) * 5,
        scratch_shapes=[
            blocks,
            blocks,
            sends,
            sends,
            blocks,
            blocks,
            sems(2 * experts),
            sems(2 * experts),
            sems(3 * PARTS),
        ],
        compiler_params=comm_params(cid),
    )(part, row_grads, third, routed, probs, gates, gain, router, routes, cotangent, target)


def gelu_parts(values):
    cdf = 0.5 * (1.0 + lax.erf(values * 0.5**0.5))
    density = jnp.exp(-0.5 * values * values) * 0.3989422804014327
    return values * cdf, cdf + values * density


def slot_targets(routes, fill_order, experts, capacity, slots):
    tokens = routes.shape[0]
    pair_expert = routes.reshape(-1)
    pair_key = (jnp.arange(2, dtype=jnp.int32)[None, :] * tokens + fill_order[:, None]).reshape(-1)
    same_expert = pair_expert[:, None] == pair_expert[None, :]
    earlier = pair_key[None, :] < pair_key[:, None]
    slot_rank = jnp.sum((same_expert & earlier).astype(jnp.int32), axis=1)
    target = jnp.where(slot_rank < capacity, pair_expert * slots + slot_rank, -1)
    return target.reshape(tokens, 2)


def dense(a, b, dims, dtype=BF16):
    return lax.dot_general(a, b, (dims, ((), ())), preferred_element_type=F32).astype(dtype)


def on_device(
    images,
    cotangent,
    key_mask,
    routes,
    fill_order,
    norm_gain1,
    qkv_weight1,
    proj_weight1,
    norm_gain2,
    fc_in,
    fc_out,
    norm_gain3,
    qkv_weight2,
    proj_weight2,
    norm_gain4,
    router,
    expert_in,
    expert_out,
):
    seq = lax.axis_size("seq")
    wide = lax.axis_size("wide")
    place = lax.axis_index("seq")
    tokens, width = images.shape[1:]
    rows = round_up(tokens, ROW_TILE)
    pad = rows - tokens
    total = seq * rows
    experts = wide // 2
    capacity = (5 * tokens + 2 * experts - 1) // (2 * experts)
    slots = round_up(capacity, ROW_TILE)
    span = width // seq
    heads = span // HEAD_DIM
    group = round_up(span, LANES)
    shard = width // wide
    units = fc_in.shape[1]
    unit_cut = units // (seq * wide)

    def gathered(x):
        return lax.all_gather(x, "wide", axis=0, tiled=True)

    def own_qkv(w):
        own = lax.dynamic_index_in_dim(w.reshape(shard, 3, seq, span), place, 2, keepdims=False)
        own = jnp.pad(own, ((0, 0), (0, 0), (0, group - span)))
        return gathered(own.reshape(shard, 3 * group))

    def own_proj(w):
        own = lax.dynamic_slice_in_dim(gathered(w), place * span, span, 0)
        return jnp.pad(own, ((0, group - span), (0, 0)))

    small = jnp.concatenate(
        [jnp.stack([norm_gain1, norm_gain2, norm_gain3, norm_gain4]), router.T], axis=0
    )
    small = lax.all_gather(small, "wide", axis=0)
    small = small.transpose(1, 0, 2).reshape(4 + experts, width)
    gains = [small[i : i + 1].astype(F32) for i in range(4)]
    router_all = jnp.pad(small[4:].T, ((0, 0), (0, LANES - experts)))

    wqkv_one = own_qkv(qkv_weight1)
    wproj_one = own_proj(proj_weight1)
    w_in = gathered(
        lax.dynamic_index_in_dim(
            fc_in.reshape(shard, wide, seq, unit_cut), place, 2, keepdims=False
        ).reshape(shard, wide * unit_cut)
    )
    w_out = gathered(lax.dynamic_slice_in_dim(fc_out, place * unit_cut, unit_cut, 0))
    wqkv_two = own_qkv(qkv_weight2)
    wproj_two = own_proj(proj_weight2)

    valid = jnp.pad(key_mask[0].reshape(seq, tokens) > 0, ((0, 0), (0, pad)))
    bias = jnp.where(valid, 0.0, -1e30).astype(F32)
    bias_row = bias.reshape(1, total)
    bias_col = bias.reshape(seq, rows, 1)
    target = jnp.pad(
        slot_targets(routes[0], fill_order[0], experts, capacity, slots),
        ((0, pad), (0, 0)),
        constant_values=-1,
    )
    routes_rows = jnp.pad(routes[0], ((0, pad), (0, 0)))
    cot = jnp.pad(cotangent[0], ((0, pad), (0, 0)))
    start = jnp.pad(images[0].astype(F32), ((0, pad), (0, 0)))

    normed_one = spread_norm(start, gains[0], tokens, 1)
    qkv_one, lse_one, mixed_one, part = attend_forward(
        normed_one, wqkv_one, wproj_one, bias_row, heads
    )
    first, normed_two = join_forward(part, start, gains[1], tokens, 2)
    flat_two = normed_two.reshape(total, width)
    pre = dense(flat_two, w_in, ((1,), (0,)), F32)
    hidden, slope = gelu_parts(pre)
    hidden, slope = hidden.astype(BF16), slope.astype(BF16)
    part = dense(hidden, w_out, ((1,), (0,))).reshape(seq, rows, width)
    second, normed_three = join_forward(part, first, gains[2], tokens, 3)
    qkv_two, lse_two, mixed_two, part = attend_forward(
        normed_three, wqkv_two, wproj_two, bias_row, heads
    )
    third, routed, probs, gates, got_rows, got_grads = dispatch(
        part, second, gains[3], router_all, routes_rows, cot, target.T, tokens, slots, 4
    )
    got_rows = got_rows.reshape(wide * slots, width)
    got_grads = got_grads.reshape(wide * slots, width)
    pre = dense(got_rows, expert_in[0], ((1,), (0,)), F32)
    e_hidden, e_slope = gelu_parts(pre)
    e_hidden = e_hidden.astype(BF16)
    e_part = dense(e_hidden, expert_out[0], ((1,), (0,)))
    e_pre = (dense(got_grads, expert_out[0], ((1,), (1,)), F32) * e_slope).astype(BF16)
    e_rows = dense(e_pre, expert_in[0], ((1,), (1,)))
    output, grad, gain4_grad, router_grad, branch = combine(
        e_part.reshape(wide, slots, width),
        e_rows.reshape(wide, slots, width),
        third,
        routed,
        probs,
        gates,
        gains[3],
        router_all,
        routes_rows,
        cot,
        target,
        tokens,
        5,
    )
    e_out_grad = dense(e_hidden, got_grads, ((0,), (0,)))
    e_in_grad = dense(got_rows, e_pre, ((0,), (0,)))

    def attention_terms(normed, mixed, branch, grad_qkv):
        gq = dense(normed.reshape(total, width), grad_qkv.reshape(total, 3 * group), ((0,), (0,)))
        gq = gq.reshape(width, 3, group)[:, :, :span].reshape(width, 3 * span)
        gp = dense(mixed.reshape(total, group)[:, :span], branch.reshape(total, width), ((0,), (0,)))
        gp = lax.all_to_all(gp, "seq", split_axis=1, concat_axis=0, tiled=True)
        return jnp.concatenate([gq, gp], axis=1)

    def reduced(terms):
        own = lax.psum_scatter(terms, "wide", scatter_dimension=0, tiled=True)
        return lax.all_gather(own, "seq", axis=0).astype(F32)

    def attention_grads(whole):
        gq = whole[:, :, : 3 * span].reshape(seq, shard, 3, span).transpose(1, 2, 0, 3)
        gp = whole[:, :, 3 * span :].transpose(1, 0, 2)
        return gq.reshape(shard, 3 * width), gp.reshape(shard, width)

    grad_qkv, part = attend_backward(
        branch, qkv_two, lse_two, mixed_two, wqkv_two, wproj_two, bias_col, heads
    )
    qkv2_grad, proj2_grad = attention_grads(
        reduced(attention_terms(normed_three, mixed_two, branch, grad_qkv))
    )
    grad, gain3_grad, branch = join_backward(part, second, gains[2], grad, tokens, 6, False)
    branch_flat = branch.reshape(total, width)
    pre_grad = (dense(branch_flat, w_out, ((1,), (1,)), F32) * slope).astype(BF16)
    part = dense(pre_grad, w_in, ((1,), (1,))).reshape(seq, rows, width)
    fc_terms = jnp.concatenate(
        [
            dense(flat_two, pre_grad, ((0,), (0,))),
            dense(hidden, branch_flat, ((0,), (0,))),
        ],
        axis=1,
    )
    fc_whole = reduced(fc_terms)
    fc_in_grad = fc_whole[:, :, : wide * unit_cut].reshape(seq, shard, wide, unit_cut)
    fc_in_grad = fc_in_grad.transpose(1, 2, 0, 3).reshape(shard, units)
    fc_out_grad = fc_whole[:, :, wide * unit_cut :].reshape(seq * unit_cut, width)
    grad, gain2_grad, branch = join_backward(part, first, gains[1], grad, tokens, 7, False)
    grad_qkv, part = attend_backward(
        branch, qkv_one, lse_one, mixed_one, wqkv_one, wproj_one, bias_col, heads
    )
    qkv1_grad, proj1_grad = attention_grads(
        reduced(attention_terms(normed_one, mixed_one, branch, grad_qkv))
    )
    image_grad, gain1_grad = join_backward(part, start, gains[0], grad, tokens, 8, True)

    small_grads = jnp.concatenate(
        [gain1_grad, gain2_grad, gain3_grad, gain4_grad, router_grad[:experts]], axis=0
    )
    small_grads = lax.psum(small_grads, ("seq", "wide"))
    small_own = lax.dynamic_slice_in_dim(
        small_grads, lax.axis_index("wide") * shard, shard, 1
    )
    e_in_all = lax.psum(e_in_grad, "seq").astype(F32)
    e_out_all = lax.psum(e_out_grad, "seq").astype(F32)
    return (
        output[None],
        image_grad[None],
        small_own[0],
        qkv1_grad,
        proj1_grad,
        small_own[1],
        fc_in_grad,
        fc_out_grad,
        small_own[2],
        qkv2_grad,
        proj2_grad,
        small_own[3],
        small_own[4:].T,
        e_in_all[None],
        e_out_all[None],
    )


def solution(mesh):
    placed = (
        P("wide", "seq", None),
        P("wide", "seq", None),
        P("wide", None),
        P("wide", "seq", None),
        P("wide", "seq"),
        P("wide"),
        P("wide", None),
        P("wide", None),
        P("wide"),
        P("wide", None),
        P("wide", None),
        P("wide"),
        P("wide", None),
        P("wide", None),
        P("wide"),
        P("wide", None),
        P("wide", None, None),
        P("wide", None, None),
    )
    return jax.shard_map(
        on_device,
        mesh=mesh,
        in_specs=placed,
        out_specs=(
            P("wide", "seq", None),
            P("wide", "seq", None),
            P("wide"),
            P("wide", None),
            P("wide", None),
            P("wide"),
            P("wide", None),
            P("wide", None),
            P("wide"),
            P("wide", None),
            P("wide", None),
            P("wide"),
            P("wide", None),
            P("wide", None, None),
            P("wide", None, None),
        ),
        check_vma=False,
    )
```

```python
import functools

import jax
import jax.numpy as jnp
from jax import lax
from jax.experimental import pallas as pl
from jax.experimental.pallas import tpu as pltpu
from jax.sharding import PartitionSpec as P

HEAD_DIM = 64
LANES = 128
ROW_TILE = 16
F32 = jnp.float32
BF16 = jnp.bfloat16
VMEM = pl.BlockSpec(memory_space=pltpu.VMEM)
ANY = pl.BlockSpec(memory_space=pl.ANY)
NT = (((1,), (1,)), ((), ()))


def round_up(n, m):
    return -(-n // m) * m


def seq_places():
    me = lax.axis_index("seq")
    near = me + 1 - 2 * lax.rem(me, 2)
    across = lax.rem(me + 2, 4)
    far = lax.rem(near + 2, 4)
    return me, near, across, far


def cuts_of(rows, parts):
    tiles = rows // ROW_TILE
    edges = [(tiles * i // parts) * ROW_TILE for i in range(parts + 1)]
    return [(a, b - a) for a, b in zip(edges[:-1], edges[1:])]


class Bank:
    def __init__(self, sems):
        self.sems, self.used = sems, 0

    def pair(self):
        self.used += 1
        return self.sems.at[0, self.used - 1], self.sems.at[1, self.used - 1]

    def remote(self, src, dst, axis, place, recv=None):
        send, own = self.pair()
        return pltpu.make_async_remote_copy(
            src_ref=src,
            dst_ref=dst,
            send_sem=send,
            recv_sem=own if recv is None else recv,
            device_id={axis: place},
            device_id_type=pl.DeviceIdType.MESH,
        )

    def local(self, src, dst):
        return pltpu.make_async_copy(src, dst, self.pair()[0])


def greet(seq_peers, wide_peers=()):
    barrier = pltpu.get_barrier_semaphore()
    for place in seq_peers:
        pl.semaphore_signal(
            barrier, inc=1, device_id={"seq": place}, device_id_type=pl.DeviceIdType.MESH
        )
    for place in wide_peers:
        pl.semaphore_signal(
            barrier, inc=1, device_id={"wide": place}, device_id_type=pl.DeviceIdType.MESH
        )
    pl.semaphore_wait(barrier, len(seq_peers) + len(wide_peers))


class RowScatter:
    def __init__(self, bank, partial, got, sent, crossed, cuts):
        self.partial, self.got, self.sent, self.crossed = partial, got, sent, crossed
        me, near, across, far = seq_places()
        self.me, self.across = me, across
        self.cuts = cuts
        self.far_part, self.near_part, self.cross = [], [], []
        for at, size in cuts:
            rows = pl.ds(at, size)
            self.far_part.append(bank.remote(partial.at[far, rows], got.at[1, rows], "seq", near))
            self.near_part.append(bank.remote(partial.at[near, rows], got.at[0, rows], "seq", near))
            self.cross.append(bank.remote(sent.at[rows], crossed.at[rows], "seq", across))

    def start(self):
        for copy in self.far_part:
            copy.start()
        for copy in self.near_part:
            copy.start()
        for i, (at, size) in enumerate(self.cuts):
            rows = pl.ds(at, size)
            self.far_part[i].wait_recv()
            self.sent[rows, :] = (
                self.partial[self.across, rows].astype(F32) + self.got[1, rows].astype(F32)
            ).astype(BF16)
            self.cross[i].start()

    def total(self, i):
        at, size = self.cuts[i]
        rows = pl.ds(at, size)
        self.near_part[i].wait_recv()
        chip = self.partial[self.me, rows].astype(F32) + self.got[0, rows].astype(F32)
        self.cross[i].wait_recv()
        return chip + self.crossed[rows, :].astype(F32)

    def finish(self):
        for copy in self.far_part + self.near_part + self.cross:
            copy.wait_send()


class RowGather:
    def __init__(self, bank, whole, cuts):
        self.whole = whole
        me, near, across, far = seq_places()
        self.me = me
        self.cuts = cuts
        self.near_copy, self.cross, self.onward = [], [], []
        for at, size in cuts:
            mine = whole.at[me, pl.ds(at, size)]
            theirs = whole.at[across, pl.ds(at, size)]
            self.near_copy.append(bank.remote(mine, mine, "seq", near))
            self.cross.append(bank.remote(mine, mine, "seq", across))
            self.onward.append(bank.remote(theirs, theirs, "seq", near))

    def send(self, i, rows):
        at, size = self.cuts[i]
        self.whole[self.me, pl.ds(at, size)] = rows
        self.cross[i].start()
        self.near_copy[i].start()

    def finish(self):
        for i in range(len(self.cuts)):
            self.cross[i].wait_recv()
            self.onward[i].start()
        for copy in self.near_copy + self.onward:
            copy.wait_recv()
        for copy in self.near_copy + self.cross + self.onward:
            copy.wait_send()


def wide_places():
    me = lax.axis_index("wide")
    half = lax.rem(me, 2)
    return me, half, me // 2, me + 1 - 2 * half


def wide_peers():
    _, half, pair, partner = wide_places()
    pairs = lax.axis_size("wide") // 2
    return [2 * lax.rem(pair + d, pairs) + half for d in range(1, pairs)] + [partner]


class Spread:
    def __init__(self, bank, src, dst):
        me, half, pair, partner = wide_places()
        pairs = lax.axis_size("wide") // 2
        self.own = bank.local(src, dst.at[me])
        self.first = [bank.remote(src, dst.at[me], "wide", p) for p in wide_peers()[:-1]]
        self.second = [bank.remote(src, dst.at[me], "wide", partner)]
        for d in range(1, pairs):
            source = 2 * lax.rem(pair + pairs - d, pairs) + half
            self.second.append(bank.remote(dst.at[source], dst.at[source], "wide", partner))

    def start(self):
        for copy in self.first:
            copy.start()
        self.second[0].start()
        self.own.start()

    def advance(self):
        for arrived, onward in zip(self.first, self.second[1:]):
            arrived.wait_recv()
            onward.start()

    def finish(self):
        for copy in self.second:
            copy.wait_recv()
        for copy in self.first + self.second:
            copy.wait_send()
        self.own.wait()


class RootSpread:
    def __init__(self, bank, src, dst):
        me, half, pair, partner = wide_places()
        self.root = pair == lax.axis_index("seq")
        landed = bank.pair()[1]
        self.own = bank.local(src, dst.at[half])
        self.out = [
            bank.remote(src, dst.at[half], "wide", p, recv=landed) for p in wide_peers()[:-1]
        ]
        self.onward = bank.remote(dst.at[half], dst.at[half], "wide", partner)

    def start(self):
        @pl.when(self.root)
        def _():
            for copy in self.out:
                copy.start()
            self.own.start()

    def advance(self):
        @pl.when(self.root)
        def _():
            self.own.wait()

        @pl.when(jnp.logical_not(self.root))
        def _():
            self.out[0].wait_recv()

        self.onward.start()

    def finish(self):
        self.onward.wait_recv()
        self.onward.wait_send()

        @pl.when(self.root)
        def _():
            for copy in self.out:
                copy.wait_send()


class Reduce:
    def __init__(self, bank, terms, came, sent, back):
        self.terms, self.came, self.sent, self.back = terms, came, sent, back
        _, self.half, self.pair, partner = wide_places()
        pairs = lax.axis_size("wide") // 2
        self.homes = [lax.rem(self.pair + d, pairs) for d in range(1, pairs)] + [self.pair]
        self.halves = [
            bank.remote(terms.at[2 * h + 1 - self.half], came.at[d], "wide", partner)
            for d, h in enumerate(self.homes)
        ]
        self.home = [
            bank.remote(sent.at[d], back.at[self.pair], "wide", 2 * h + self.half)
            for d, h in enumerate(self.homes[:-1])
        ]

    def start(self):
        for copy in self.halves:
            copy.start()

    def advance(self):
        for d, h in enumerate(self.homes):
            self.halves[d].wait_recv()
            both = self.terms[2 * h + self.half].astype(F32) + self.came[d].astype(F32)
            if d < len(self.home):
                self.sent[d] = both.astype(self.sent.dtype)
                self.home[d].start()
            else:
                self.back[self.pair] = both.astype(self.back.dtype)

    def total(self):
        for copy in self.home:
            copy.wait_recv()
        total = self.back[0].astype(F32)
        for p in range(1, self.back.shape[0]):
            total = total + self.back[p].astype(F32)
        return total

    def finish(self):
        for copy in self.halves + self.home:
            copy.wait_send()


class RootReduce:
    def __init__(self, bank, terms, came, sent, back, low, out):
        self.terms, self.came, self.sent, self.back = terms, came, sent, back
        self.low = low
        _, self.half, self.pair, partner = wide_places()
        me, near, across, far = seq_places()
        pairs = lax.axis_size("wide") // 2
        self.root = self.pair == me
        self.halves = bank.remote(terms.at[1 - self.half], came, "wide", partner)
        self.to_root = []
        for d in range(1, pairs):
            place = lax.rem(self.pair + d, pairs)
            copy = bank.remote(sent, back.at[self.pair], "wide", 2 * place + self.half)
            self.to_root.append((place == me, copy))
        landed = bank.pair()[1]
        self.own = bank.local(low, out)
        self.cast = [bank.remote(low, out, "seq", p, recv=landed) for p in (across, far, near)]

    def start(self):
        self.halves.start()

    def advance(self):
        self.halves.wait_recv()
        both = (self.terms[self.half].astype(F32) + self.came[...].astype(F32)).astype(BF16)
        self.sent[...] = both

        @pl.when(self.root)
        def _():
            self.back[self.pair] = both

        for mine, copy in self.to_root:

            @pl.when(mine)
            def _():
                copy.start()

    def settle(self):
        @pl.when(self.root)
        def _():
            for _, copy in self.to_root:
                copy.wait_recv()
            total = self.back[0].astype(F32)
            for p in range(1, self.back.shape[0]):
                total = total + self.back[p].astype(F32)
            self.low[...] = total.astype(BF16)
            for copy in self.cast:
                copy.start()
            self.own.start()

    def finish(self):
        self.halves.wait_send()
        for mine, copy in self.to_root:

            @pl.when(mine)
            def _():
                copy.wait_send()

        @pl.when(self.root)
        def _():
            for copy in self.cast:
                copy.wait_send()
            self.own.wait()

        @pl.when(jnp.logical_not(self.root))
        def _():
            self.cast[0].wait_recv()


class BlockGather:
    def __init__(self, bank, src, whole):
        me, near, across, far = seq_places()
        self.own = bank.local(src, whole.at[me])
        self.near_copy = bank.remote(src, whole.at[me], "seq", near)
        self.cross = bank.remote(src, whole.at[me], "seq", across)
        self.onward = bank.remote(whole.at[across], whole.at[across], "seq", near)

    def start(self):
        self.cross.start()
        self.near_copy.start()
        self.own.start()

    def advance(self):
        self.cross.wait_recv()
        self.onward.start()

    def finish(self):
        self.near_copy.wait_recv()
        self.onward.wait_recv()
        self.own.wait()
        for copy in (self.near_copy, self.cross, self.onward):
            copy.wait_send()


class Task:
    def __init__(self, ins, outs, scratch, make):
        self.ins, self.outs, self.scratch, self.make = ins, outs, scratch, make


def like(x):
    return jax.ShapeDtypeStruct(x.shape, x.dtype)


def spread_task(block, view=lambda ref: ref, shape=None):
    shape = block.shape if shape is None else shape
    wide = lax.axis_size("wide")
    return Task(
        [(block, VMEM)],
        [(jax.ShapeDtypeStruct((wide, *shape), block.dtype), ANY)],
        [],
        lambda bank, ins, outs, scratch: Spread(bank, view(ins[0]), outs[0]),
    )


def root_spread_task(block):
    return Task(
        [(block, VMEM)],
        [(jax.ShapeDtypeStruct((2, *block.shape), block.dtype), ANY)],
        [],
        lambda bank, ins, outs, scratch: RootSpread(bank, ins[0], outs[0]),
    )


def reduce_scratch(block, dtype=BF16):
    pairs = lax.axis_size("wide") // 2
    return [
        pltpu.VMEM((pairs, *block), dtype),
        pltpu.VMEM((max(pairs - 1, 1), *block), dtype),
        pltpu.VMEM((pairs, *block), dtype),
    ]


class ReduceOut(Reduce):
    def __init__(self, bank, terms, out, scratch):
        super().__init__(bank, terms, *scratch)
        self.out = out

    def finish(self):
        self.out[...] = self.total().astype(BF16)
        super().finish()


def reduce_task(terms):
    return Task(
        [(terms, VMEM)],
        [(jax.ShapeDtypeStruct(terms.shape[1:], BF16), VMEM)],
        reduce_scratch(terms.shape[1:]),
        lambda bank, ins, outs, scratch: ReduceOut(bank, ins[0], outs[0], scratch),
    )


class RootReduceOut(RootReduce):
    def finish(self):
        self.settle()
        super().finish()


def root_reduce_task(terms):
    block = terms.shape[1:]
    pairs = lax.axis_size("wide") // 2
    one = pltpu.VMEM(block, BF16)
    return Task(
        [(terms, VMEM)],
        [(jax.ShapeDtypeStruct(block, BF16), ANY)],
        [one, one, pltpu.VMEM((pairs, *block), BF16), one],
        lambda bank, ins, outs, scratch: RootReduceOut(bank, ins[0], *scratch, outs[0]),
    )


def block_gather_task(block):
    return Task(
        [(block, VMEM)],
        [(jax.ShapeDtypeStruct((4, *block.shape), block.dtype), ANY)],
        [],
        lambda bank, ins, outs, scratch: BlockGather(bank, ins[0], outs[0]),
    )


MAX_COPIES = 96


def call(body, ins, outs, scratch, tasks=(), cid=None, grid=None):
    all_ins, all_outs, all_scratch = list(ins), list(outs), list(scratch)
    for task in tasks:
        all_ins += task.ins
        all_outs += task.outs
        all_scratch += task.scratch
    remote = cid is not None
    if remote:
        all_scratch.append(pltpu.SemaphoreType.DMA((2, MAX_COPIES)))

    def kernel(*refs):
        refs = list(refs)
        groups = []
        for count, key in ((len(ins), "ins"), (len(outs), "outs"), (len(scratch), "scratch")):
            own, refs = refs[:count], refs[count:]
            of_tasks = []
            for task in tasks:
                n = len(getattr(task, key))
                of_tasks.append(refs[:n])
                refs = refs[n:]
            groups.append((own, of_tasks))
        bank = Bank(refs[0]) if remote else None
        live = [
            task.make(bank, groups[0][1][i], groups[1][1][i], groups[2][1][i])
            for i, task in enumerate(tasks)
        ]
        body(groups[0][0], groups[1][0], groups[2][0], bank, live)

    params = {}
    if remote:
        params = dict(collective_id=cid, has_side_effects=True)
    extra = {}
    if grid is not None:
        params["dimension_semantics"] = ("arbitrary",)
        extra["grid"] = grid
    return pl.pallas_call(
        kernel,
        out_shape=tuple(shape for shape, _ in all_outs),
        in_specs=[spec for _, spec in all_ins],
        out_specs=tuple(spec for _, spec in all_outs),
        scratch_shapes=all_scratch,
        compiler_params=pltpu.CompilerParams(**params),
        **extra,
    )(*[x for x, _ in all_ins])


def meet(tasks, far=False):
    _, near, across, beyond = seq_places()
    greet((near, across) + ((beyond,) if far else ()), wide_peers() if tasks else ())


def real_rows(at, size, tokens):
    return at + lax.broadcasted_iota(jnp.int32, (size, 1), 0) < tokens


def centre(values):
    centred = values - jnp.mean(values, axis=-1, keepdims=True)
    variance = jnp.mean(centred * centred, axis=-1, keepdims=True)
    scale = lax.rsqrt(variance + 1e-06)
    return centred * scale, scale


def norm_forward(values, gain):
    return centre(values)[0] * gain


def norm_backward(values, gain, grad):
    unit, scale = centre(values)
    grad_unit = grad * gain
    grad_in = scale * (
        grad_unit
        - jnp.mean(grad_unit, axis=-1, keepdims=True)
        - unit * jnp.mean(grad_unit * unit, axis=-1, keepdims=True)
    )
    return grad_in, jnp.sum(grad * unit, axis=0, keepdims=True)


def scatter_scratch(rows, width):
    return [
        pltpu.VMEM((2, rows, width), BF16),
        pltpu.VMEM((rows, width), BF16),
        pltpu.VMEM((rows, width), BF16),
    ]


PARTS = 2


def spread_norm(residual, gains, tokens, cid):
    rows, width = residual.shape
    cuts = cuts_of(rows, PARTS)

    def body(ins, outs, scratch, bank, tasks):
        residual_ref, gains_ref = ins
        gather = RowGather(bank, outs[0], cuts)
        meet(tasks)
        for i, (at, size) in enumerate(cuts):
            normed = norm_forward(residual_ref[pl.ds(at, size), :], gains_ref[0:1, :])
            normed = jnp.where(real_rows(at, size, tokens), normed, 0.0)
            gather.send(i, normed.astype(BF16))
        gather.finish()

    return call(
        body,
        [(residual, VMEM), (gains, VMEM)],
        [(jax.ShapeDtypeStruct((4, rows, width), BF16), VMEM)],
        [],
        cid=cid,
    )[0]


def own_columns(ref, parts, span, group, place):
    rows = ref.shape[0]
    width = ref.shape[1] // parts
    blocks = []
    for part in range(parts):
        own = jnp.zeros((rows, span), F32)
        for s in range(width // span):
            at = part * width + s * span
            own = jnp.where(place == s, ref[:, at : at + span].astype(F32), own)
        blocks.append((part * group, own))
    return blocks


def own_units(ref, place, seq):
    rows = ref.shape[0]
    cut = LANES // seq
    lane = lax.broadcasted_iota(jnp.int32, (rows, LANES), 1)
    tiles = []
    for tile in range(ref.shape[1] // (seq * LANES)):
        own = jnp.zeros((rows, LANES), F32)
        for q in range(seq):
            at = (tile * seq + q) * LANES
            shift = lax.rem(cut * q + LANES - cut * place, LANES)
            turned = pltpu.roll(ref[:, at : at + LANES].astype(F32), shift, 1)
            own = jnp.where(lane // cut == q, turned, own)
        tiles.append(own)
    return tiles


def begin(residual, small, qkv_one, proj_one, qkv_two, fc_in, tokens, span, group, cid):
    rows, width = residual.shape
    shard = qkv_one.shape[0]
    wide = lax.axis_size("wide")
    seq = lax.axis_size("seq")
    cuts = cuts_of(rows, PARTS)
    units = fc_in.shape[1] // seq

    def body(ins, outs, scratch, bank, tasks):
        residual_ref, small_ref, qkv1_ref, proj1_ref, qkv2_ref, fc_ref = ins
        whole_ref, gains_ref, router_ref, qkv2_own, fc_own, wqkv_ref, wproj_ref = outs
        small_all, own_ref = scratch
        place = lax.axis_index("seq")
        gather = RowGather(bank, whole_ref, cuts)
        smalls = Spread(bank, small_ref, small_all)
        weights = Spread(bank, own_ref, wqkv_ref)
        proj = RootSpread(bank, proj1_ref, wproj_ref)
        _, near, across, _ = seq_places()
        greet((near, across), wide_peers())
        smalls.start()
        own_ref[...] = jnp.zeros_like(own_ref)
        for at, own in own_columns(qkv1_ref, 3, span, group, place):
            own_ref[:, at : at + span] = own.astype(BF16)
        weights.start()
        proj.start()
        smalls.advance()
        smalls.finish()
        column = lax.broadcasted_iota(jnp.int32, (LANES, width), 1)
        lane = lax.broadcasted_iota(jnp.int32, (LANES, width), 0)
        joined = jnp.zeros((small_ref.shape[0], width), F32)
        for w in range(wide):
            spot = ((column == lane + w * shard) & (lane < shard)).astype(F32).astype(BF16)
            joined += jnp.dot(small_all[w], spot, preferred_element_type=F32)
        gains_ref[...] = joined
        experts = wide // 2
        router_ref[...] = jnp.zeros_like(router_ref)
        router_ref[0 : joined.shape[0], :] = jnp.concatenate(
            [joined[4:], jnp.zeros((4, width), F32)], axis=0
        ).astype(BF16)
        for i, (at, size) in enumerate(cuts):
            normed = norm_forward(residual_ref[pl.ds(at, size), :], gains_ref[0:1, :])
            normed = jnp.where(real_rows(at, size, tokens), normed, 0.0)
            gather.send(i, normed.astype(BF16))
        proj.advance()
        weights.advance()
        qkv2_own[...] = jnp.zeros_like(qkv2_own)
        for at, own in own_columns(qkv2_ref, 3, span, group, place):
            qkv2_own[:, at : at + span] = own.astype(BF16)
        for tile, own in enumerate(own_units(fc_ref, place, seq)):
            fc_own[:, tile * LANES : (tile + 1) * LANES] = own.astype(BF16)
        gather.finish()
        proj.finish()
        weights.finish()

    shape = jax.ShapeDtypeStruct
    return call(
        body,
        [(x, VMEM) for x in (residual, small, qkv_one, proj_one, qkv_two, fc_in)],
        [
            (shape((4, rows, width), BF16), VMEM),
            (shape((small.shape[0], width), F32), VMEM),
            (shape((LANES, width), BF16), VMEM),
            (shape((shard, 3 * group), BF16), VMEM),
            (shape((shard, units), BF16), VMEM),
            (shape((wide, shard, 3 * group), BF16), ANY),
            (shape((2, shard, width), BF16), ANY),
        ],
        [
            pltpu.VMEM((wide, *small.shape), BF16),
            pltpu.VMEM((shard, 3 * group), BF16),
        ],
        cid=cid,
    )


def join_forward(partial, residual, gains, which, tokens, cid, tasks=()):
    rows, width = residual.shape
    cuts = cuts_of(rows, PARTS)

    def body(ins, outs, scratch, bank, tasks):
        partial_ref, residual_ref, gains_ref = ins
        out_ref, whole_ref = outs
        scatter = RowScatter(bank, partial_ref, *scratch, cuts)
        gather = RowGather(bank, whole_ref, cuts)
        meet(tasks)
        for task in tasks:
            task.start()
        scatter.start()
        for i, (at, size) in enumerate(cuts):
            total = residual_ref[pl.ds(at, size), :] + scatter.total(i)
            out_ref[pl.ds(at, size), :] = total
            normed = norm_forward(total, gains_ref[which : which + 1, :])
            normed = jnp.where(real_rows(at, size, tokens), normed, 0.0)
            gather.send(i, normed.astype(BF16))
        for task in tasks:
            task.advance()
        gather.finish()
        scatter.finish()
        for task in tasks:
            task.finish()

    return call(
        body,
        [(partial, VMEM), (residual, VMEM), (gains, VMEM)],
        [
            (jax.ShapeDtypeStruct((rows, width), F32), VMEM),
            (jax.ShapeDtypeStruct((4, rows, width), BF16), VMEM),
        ],
        scatter_scratch(rows, width),
        tasks,
        cid,
    )


def join_backward(partial, residual, gains, which, grad, tokens, cid, tasks=()):
    rows, width = residual.shape
    cuts = cuts_of(rows, PARTS)

    def body(ins, outs, scratch, bank, tasks):
        partial_ref, residual_ref, gains_ref, grad_ref = ins
        out_ref, gain_grad_ref, whole_ref = outs
        gather = RowGather(bank, whole_ref, cuts)
        scatter = RowScatter(bank, partial_ref, *scratch, cuts)
        meet(tasks, far=bool(tasks))
        for task in tasks:
            task.start()
        scatter.start()
        gain_grad = jnp.zeros((1, width), F32)
        for i, (at, size) in enumerate(cuts):
            rows_here = pl.ds(at, size)
            grad_in, term = norm_backward(
                residual_ref[rows_here, :], gains_ref[which : which + 1, :], scatter.total(i)
            )
            gain_grad = gain_grad + term
            grad_out = grad_ref[rows_here, :] + grad_in
            out_ref[rows_here, :] = grad_out
            gather.send(i, grad_out.astype(BF16))
        gain_grad_ref[...] = gain_grad
        for task in tasks:
            task.advance()
        gather.finish()
        scatter.finish()
        for task in tasks:
            task.finish()

    return call(
        body,
        [(partial, VMEM), (residual, VMEM), (gains, VMEM), (grad, VMEM)],
        [
            (jax.ShapeDtypeStruct((rows, width), F32), VMEM),
            (jax.ShapeDtypeStruct((1, width), F32), VMEM),
            (jax.ShapeDtypeStruct((4, rows, width), BF16), VMEM),
        ],
        scatter_scratch(rows, width),
        tasks,
        cid,
    )


def close_plain(partial, residual, gains, grad, tokens, cid):
    rows, width = residual.shape
    cuts = cuts_of(rows, PARTS)

    def body(ins, outs, scratch, bank, tasks):
        partial_ref, residual_ref, gains_ref, grad_ref = ins
        out_ref, gain_grad_ref = outs
        scatter = RowScatter(bank, partial_ref, *scratch, cuts)
        meet(tasks)
        scatter.start()
        gain_grad = jnp.zeros((1, width), F32)
        for i, (at, size) in enumerate(cuts):
            rows_here = pl.ds(at, size)
            grad_in, term = norm_backward(
                residual_ref[rows_here, :], gains_ref[0:1, :], scatter.total(i)
            )
            gain_grad = gain_grad + term
            keep = min(size, tokens - at)
            out_ref[pl.ds(at, keep), :] = (grad_ref[rows_here, :] + grad_in)[:keep]
        gain_grad_ref[...] = gain_grad
        scatter.finish()

    return call(
        body,
        [(partial, VMEM), (residual, VMEM), (gains, VMEM), (grad, VMEM)],
        [
            (jax.ShapeDtypeStruct((tokens, width), F32), VMEM),
            (jax.ShapeDtypeStruct((1, width), F32), VMEM),
        ],
        scatter_scratch(rows, width),
        cid=cid,
    )


def close(partial, residual, gains, grad, smalls, qkv_terms, proj_terms, fc_block, tokens, cid):
    rows, width = residual.shape
    cuts = cuts_of(rows, PARTS)
    wide = lax.axis_size("wide")
    shard = qkv_terms.shape[1]
    block = qkv_terms.shape[1:]
    small_rows = ROW_TILE

    def body(ins, outs, scratch, bank, tasks):
        partial_ref, residual_ref, gains_ref, grad_ref, smalls_ref, terms_ref, fc_ref = ins
        out_ref, small_ref, qkv_ref, fc_all = outs
        scatter = RowScatter(bank, partial_ref, *scratch[:3], cuts)
        reduce = Reduce(bank, terms_ref, *scratch[3:6])
        low_ref = scratch[6]
        small_terms = scratch[7]
        small = Reduce(bank, small_terms, *scratch[8:11])
        mine, met, both, crossed = scratch[11:15]
        _, near, across, far = seq_places()
        spread = BlockGather(bank, low_ref, qkv_ref)
        fc = BlockGather(bank, fc_ref, fc_all)
        to_near = bank.remote(mine, met, "seq", near)
        to_across = bank.remote(both, crossed, "seq", across)
        greet((near, across, far), wide_peers())
        for task in tasks:
            task.start()
        reduce.start()
        scatter.start()
        gain_grad = jnp.zeros((1, width), F32)
        for i, (at, size) in enumerate(cuts):
            rows_here = pl.ds(at, size)
            grad_in, term = norm_backward(
                residual_ref[rows_here, :], gains_ref[0:1, :], scatter.total(i)
            )
            gain_grad = gain_grad + term
            keep = min(size, tokens - at)
            out_ref[pl.ds(at, keep), :] = (grad_ref[rows_here, :] + grad_in)[:keep]
        fc.start()
        terms = jnp.concatenate(
            [gain_grad, smalls_ref[...], jnp.zeros((small_rows - 1 - smalls_ref.shape[0], width), F32)],
            axis=0,
        )
        high = terms.astype(BF16)
        rest = (terms - high.astype(F32)).astype(BF16)
        column = lax.broadcasted_iota(jnp.int32, (LANES, width), 1)
        lane = lax.broadcasted_iota(jnp.int32, (LANES, width), 0)
        for w in range(wide):
            spot = ((column == lane + w * shard) & (lane < shard)).astype(F32).astype(BF16)
            small_terms[w] = lax.dot_general(
                high, spot, NT, preferred_element_type=F32
            ) + lax.dot_general(rest, spot, NT, preferred_element_type=F32)
        small.start()
        for task in tasks:
            task.advance()
        reduce.advance()
        small.advance()
        fc.advance()
        low_ref[...] = reduce.total().astype(BF16)
        spread.start()
        mine[...] = small.total()
        to_near.start()
        for task in tasks:
            task.settle()
        to_near.wait_recv()
        both[...] = mine[...] + met[...]
        to_across.start()
        spread.advance()
        to_across.wait_recv()
        small_ref[...] = both[...] + crossed[...]
        scatter.finish()
        reduce.finish()
        small.finish()
        fc.finish()
        spread.finish()
        for task in tasks:
            task.finish()
        to_near.wait_send()
        to_across.wait_send()

    shape = jax.ShapeDtypeStruct
    small_block = pltpu.VMEM((small_rows, LANES), F32)
    root = root_reduce_task(proj_terms)
    root.make = lambda bank, ins, outs, scratch: RootReduce(bank, ins[0], *scratch, outs[0])
    return call(
        body,
        [
            (x, VMEM)
            for x in (partial, residual, gains, grad, smalls, qkv_terms, fc_block)
        ],
        [
            (shape((tokens, width), F32), VMEM),
            (shape((small_rows, LANES), F32), VMEM),
            (shape((4, *block), BF16), ANY),
            (shape((4, *fc_block.shape), BF16), ANY),
        ],
        scatter_scratch(rows, width)
        + reduce_scratch(block)
        + [pltpu.VMEM(block, BF16), pltpu.VMEM((wide, small_rows, LANES), F32)]
        + reduce_scratch((small_rows, LANES), F32)
        + [small_block] * 4,
        [root],
        cid,
    )


def assemble(qkv_one, qkv_two, fc_in, fc_out, proj_one, proj_two, span, group):
    seq, shard, _ = qkv_one.shape
    width = proj_one.shape[1]
    cut = LANES // seq
    tiles = fc_in.shape[2] // LANES

    def body(ins, outs, scratch, bank, tasks):
        for src, out in zip(ins[:2], outs[:2]):
            for part in range(3):
                for s in range(seq):
                    at = part * width + s * span
                    out[:, at : at + span] = src[s, :, part * group : part * group + span].astype(
                        F32
                    )
        lane = lax.broadcasted_iota(jnp.int32, (shard, LANES), 1)
        for tile in range(tiles):
            pieces = [
                ins[2][s, :, tile * LANES : (tile + 1) * LANES].astype(F32) for s in range(seq)
            ]
            for q in range(seq):
                own = jnp.zeros((shard, LANES), F32)
                for s in range(seq):
                    turned = pieces[s]
                    if s != q:
                        turned = pltpu.roll(turned, (cut * (s - q)) % LANES, 1)
                    own = jnp.where(lane // cut == s, turned, own)
                at = (tile * seq + q) * LANES
                outs[2][:, at : at + LANES] = own
        for s in range(seq):
            for g in range(fc_out.shape[1] // cut):
                outs[3][pl.ds(g * LANES + s * cut, cut), :] = ins[3][s, pl.ds(g * cut, cut), :].astype(
                    F32
                )
        outs[4][...] = ins[4][...].astype(F32)
        outs[5][...] = ins[5][...].astype(F32)

    shape = jax.ShapeDtypeStruct
    return call(
        body,
        [(x, VMEM) for x in (qkv_one, qkv_two, fc_in, fc_out, proj_one, proj_two)],
        [
            (shape((shard, 3 * width), F32), VMEM),
            (shape((shard, 3 * width), F32), VMEM),
            (shape((shard, seq * fc_in.shape[2]), F32), VMEM),
            (shape((seq * fc_out.shape[1], width), F32), VMEM),
            (shape((shard, width), F32), VMEM),
            (shape((shard, width), F32), VMEM),
        ],
        [],
    )


def head_lanes(rows, head):
    lane = lax.broadcasted_iota(jnp.int32, (rows, LANES), 1)
    low = (head % 2) * HEAD_DIM
    return (lane >= low) & (lane < low + HEAD_DIM)


def kept(*shape):
    return pl.BlockSpec(shape, lambda i: (0,) * len(shape))


def padded_rows(ref, src, span):
    ref[0:span, :] = src[...].reshape(span, src.shape[-1])
    ref[span:, :] = jnp.zeros((ref.shape[0] - span, ref.shape[1]), ref.dtype)


def attend_forward(normed_all, wqkv, wproj, bias_row, heads, cid=None, tasks=()):
    blocks, rows, width = normed_all.shape
    group = wqkv.shape[1] // 3
    span = heads * HEAD_DIM
    total = blocks * rows

    def body(ins, outs, scratch, bank, tasks):
        normed_ref, wqkv_ref, wproj_in, bias_ref = ins
        qkv_ref, lse_ref, mixed_ref, part_ref = outs
        (wproj_ref,) = scratch
        step = pl.program_id(0)

        @pl.when(step == 0)
        def _():
            if tasks:
                meet(tasks)
            for task in tasks:
                task.start()
            padded_rows(wproj_ref, wproj_in, span)

            @pl.loop(0, blocks)
            def _(b):
                qkv_ref[b] = jnp.dot(
                    normed_ref[b], wqkv_ref[...], preferred_element_type=F32
                ).astype(BF16)

        lane = lax.broadcasted_iota(jnp.int32, (rows, LANES), 1)
        lse = jnp.zeros((rows, LANES), F32)
        for pair in range(group // LANES):
            lo = pair * LANES
            query = qkv_ref[step, :, lo : lo + LANES].astype(F32) * HEAD_DIM ** (-0.5)
            keys = qkv_ref[:, :, group + lo : group + lo + LANES].reshape(total, LANES)
            values = qkv_ref[:, :, 2 * group + lo : 2 * group + lo + LANES].reshape(total, LANES)
            mixed = jnp.zeros((rows, LANES), F32)
            for head in range(2 * pair, min(2 * pair + 2, heads)):
                mine = head_lanes(rows, head)
                scores = lax.dot_general(
                    jnp.where(mine, query, 0.0).astype(BF16), keys, NT, preferred_element_type=F32
                )
                scores = scores + bias_ref[...]
                peak = jnp.max(scores, axis=-1, keepdims=True)
                exps = jnp.exp(scores - peak)
                row_total = jnp.sum(exps, axis=-1, keepdims=True)
                out = jnp.dot(exps.astype(BF16), values, preferred_element_type=F32)
                mixed = jnp.where(mine, out / row_total, mixed)
                lse = jnp.where(lane == head, peak + jnp.log(row_total), lse)
            mixed_ref[step, :, lo : lo + LANES] = mixed.astype(BF16)
        lse_ref[step] = lse
        part_ref[step] = jnp.dot(
            mixed_ref[step], wproj_ref[...], preferred_element_type=F32
        ).astype(BF16)

        if tasks:

            @pl.when(step == blocks - 2)
            def _():
                for task in tasks:
                    task.advance()

            @pl.when(step == blocks - 1)
            def _():
                for task in tasks:
                    task.finish()

    shape = jax.ShapeDtypeStruct
    return call(
        body,
        [
            (normed_all, kept(blocks, rows, width)),
            (wqkv, kept(width, 3 * group)),
            (wproj, kept(*wproj.shape)),
            (bias_row, kept(1, total)),
        ],
        [
            (shape((blocks, rows, 3 * group), BF16), kept(blocks, rows, 3 * group)),
            (shape((blocks, rows, LANES), F32), kept(blocks, rows, LANES)),
            (shape((blocks, rows, group), BF16), kept(blocks, rows, group)),
            (shape((blocks, rows, width), BF16), kept(blocks, rows, width)),
        ],
        [pltpu.VMEM((group, width), BF16)],
        tasks,
        cid,
        (blocks,),
    )


def attend_backward(branch_all, qkv, lse, mixed, wqkv, wproj, bias_col, heads, cid=None, tasks=()):
    blocks, rows, width = branch_all.shape
    group = wqkv.shape[1] // 3
    span = heads * HEAD_DIM
    pairs = group // LANES
    total = blocks * rows

    def body(ins, outs, scratch, bank, tasks):
        branch_ref, qkv_ref, lse_ref, mixed_ref, wqkv_ref, wproj_in, bias_ref = ins
        grad_ref, part_ref = outs
        gm_ref, query_ref, grads_ref, stats_ref, dq_ref, wproj_ref = scratch
        step = pl.program_id(0)

        @pl.when(step == 0)
        def _():
            if tasks:
                meet(tasks)
            for task in tasks:
                task.start()
            padded_rows(wproj_ref, wproj_in, span)

            @pl.loop(0, blocks)
            def _(b):
                gm_ref[b] = lax.dot_general(
                    branch_ref[b], wproj_ref[...], NT, preferred_element_type=F32
                ).astype(BF16)

            lse_rows = lse_ref[...].reshape(total, LANES).T
            for head in range(heads):
                lo = (head // 2) * LANES
                mine = head_lanes(total, head)
                query = qkv_ref[:, :, lo : lo + LANES].reshape(total, LANES).astype(F32)
                query_ref[head] = jnp.where(mine, query * HEAD_DIM ** (-0.5), 0.0).astype(BF16)
                grads = gm_ref[:, :, lo : lo + LANES].reshape(total, LANES).astype(F32)
                grads = jnp.where(mine, grads, 0.0)
                grads_ref[head] = grads.astype(BF16)
                out = mixed_ref[:, :, lo : lo + LANES].reshape(total, LANES).astype(F32)
                stats_ref[head] = jnp.concatenate(
                    [
                        lse_rows[head : head + 1],
                        jnp.sum((grads * out).T, axis=0, keepdims=True),
                        jnp.zeros((6, total), F32),
                    ],
                    axis=0,
                )
            dq_ref[...] = jnp.zeros_like(dq_ref)

        for pair in range(pairs):
            lo = pair * LANES
            keys = qkv_ref[step, :, group + lo : group + lo + LANES]
            values = qkv_ref[step, :, 2 * group + lo : 2 * group + lo + LANES]
            grad_keys = jnp.zeros((rows, LANES), F32)
            grad_values = jnp.zeros((rows, LANES), F32)
            for head in range(2 * pair, min(2 * pair + 2, heads)):
                scores = lax.dot_general(keys, query_ref[head], NT, preferred_element_type=F32)
                probs = jnp.exp(scores + bias_ref[step] - stats_ref[head, 0:1])
                grad_probs = lax.dot_general(
                    values, grads_ref[head], NT, preferred_element_type=F32
                )
                grad_scores = (probs * (grad_probs - stats_ref[head, 1:2])).astype(BF16)
                grad_values += jnp.dot(
                    probs.astype(BF16), grads_ref[head], preferred_element_type=F32
                )
                grad_keys += jnp.dot(grad_scores, query_ref[head], preferred_element_type=F32)
                mine = head_lanes(rows, head)
                own_keys = jnp.where(mine, keys.astype(F32), 0.0).T.astype(BF16)
                dq_ref[pl.ds(lo, LANES), :] += jnp.dot(
                    own_keys, grad_scores, preferred_element_type=F32
                )
            grad_ref[step, :, group + lo : group + lo + LANES] = grad_keys.astype(BF16)
            grad_ref[step, :, 2 * group + lo : 2 * group + lo + LANES] = grad_values.astype(BF16)

        if tasks:

            @pl.when(step == blocks - 2)
            def _():
                for task in tasks:
                    task.advance()

        @pl.when(step == blocks - 1)
        def _():
            for pair in range(pairs):
                lo = pair * LANES
                grad_query = dq_ref[pl.ds(lo, LANES), :].T * HEAD_DIM ** (-0.5)
                grad_ref[:, :, lo : lo + LANES] = grad_query.astype(BF16).reshape(
                    blocks, rows, LANES
                )

            @pl.loop(0, blocks)
            def _(b):
                part_ref[b] = lax.dot_general(
                    grad_ref[b], wqkv_ref[...], NT, preferred_element_type=F32
                ).astype(BF16)

            for task in tasks:
                task.finish()

    shape = jax.ShapeDtypeStruct
    return call(
        body,
        [
            (branch_all, kept(blocks, rows, width)),
            (qkv, kept(blocks, rows, 3 * group)),
            (lse, kept(blocks, rows, LANES)),
            (mixed, kept(blocks, rows, group)),
            (wqkv, kept(width, 3 * group)),
            (wproj, kept(*wproj.shape)),
            (bias_col, kept(blocks, rows, 1)),
        ],
        [
            (shape((blocks, rows, 3 * group), BF16), kept(blocks, rows, 3 * group)),
            (shape((blocks, rows, width), BF16), kept(blocks, rows, width)),
        ],
        [
            pltpu.VMEM((blocks, rows, group), BF16),
            pltpu.VMEM((heads, total, LANES), BF16),
            pltpu.VMEM((heads, total, LANES), BF16),
            pltpu.VMEM((heads, 8, total), F32),
            pltpu.VMEM((group, total), F32),
            pltpu.VMEM((group, width), BF16),
        ],
        tasks,
        cid,
        (blocks,),
    )


def dispatch(partial, residual, gains, router, routes, cotangent, target, tokens, slots, cid):
    rows, width = residual.shape
    wide = lax.axis_size("wide")
    experts = wide // 2
    cuts = cuts_of(rows, PARTS)

    def kernel(
        partial_ref,
        residual_ref,
        gain_ref,
        router_ref,
        routes_ref,
        cot_ref,
        target_ref,
        third_ref,
        routed_ref,
        probs_ref,
        gates_ref,
        rows_ref,
        grads_ref,
        got,
        sent,
        crossed,
        send_rows,
        send_grads,
        gated_ref,
        all_sems,
    ):
        bank = Bank(all_sems)
        _, near, across, _ = seq_places()
        me, half, expert, partner = wide_places()
        scatter = RowScatter(bank, partial_ref, got, sent, crossed, cuts)
        others = [lax.rem(expert + d, experts) for d in range(1, experts)]
        greet((near, across), [2 * e + half for e in others] + [partner])
        scatter.start()
        for i, (at, size) in enumerate(cuts):
            here = pl.ds(at, size)
            total = residual_ref[here, :] + scatter.total(i)
            third_ref[here, :] = total
            normed = norm_forward(total, gain_ref[3:4, :])
            normed = jnp.where(real_rows(at, size, tokens), normed, 0.0)
            routed_ref[here, :] = normed.astype(BF16)
        scatter.finish()

        slot = lax.broadcasted_iota(jnp.int32, (slots, rows), 0)

        def chosen(e, k):
            return (slot + e * slots == target_ref[k : k + 1, :]).astype(F32)

        def exchange(block_of, send, out):
            first = []
            for d, e in enumerate(others):
                send[d] = block_of(e)
                first.append(bank.remote(send.at[d], out.at[me], "wide", 2 * e + half))
                first[-1].start()
            out[me] = block_of(expert)
            return first

        def pass_on(first, out):
            second = [bank.remote(out.at[me], out.at[me], "wide", partner)]
            second[0].start()
            for d in range(1, experts):
                first[d - 1].wait_recv()
                source = 2 * lax.rem(expert + experts - d, experts) + half
                second.append(bank.remote(out.at[source], out.at[source], "wide", partner))
                second[-1].start()
            return second

        def row_block(e):
            pick = (chosen(e, 0) + chosen(e, 1)).astype(BF16)
            return jnp.dot(pick, routed_ref[...], preferred_element_type=F32).astype(BF16)

        first_rows = exchange(row_block, send_rows, rows_ref)

        lane = lax.broadcasted_iota(jnp.int32, (rows, LANES), 1)
        logits = lax.dot_general(
            routed_ref[...], router_ref[...], NT, preferred_element_type=F32
        )
        logits = jnp.where(lane < experts, logits, -1e30)
        exps = jnp.exp(logits - jnp.max(logits, axis=-1, keepdims=True))
        probs = exps / jnp.sum(exps, axis=-1, keepdims=True)
        probs_ref[...] = probs
        gates = jnp.zeros((rows, LANES), F32)
        for k in range(2):
            gate = jnp.sum(
                jnp.where(lane == routes_ref[:, k : k + 1], probs, 0.0), axis=-1, keepdims=True
            )
            gates = jnp.where(lane == k, gate, gates)
            gated_ref[k] = (gate * cot_ref[...].astype(F32)).astype(BF16)
        gates_ref[...] = gates

        def grad_block(e):
            both = jnp.dot(chosen(e, 0).astype(BF16), gated_ref[0], preferred_element_type=F32)
            both += jnp.dot(chosen(e, 1).astype(BF16), gated_ref[1], preferred_element_type=F32)
            return both.astype(BF16)

        first_grads = exchange(grad_block, send_grads, grads_ref)
        second = pass_on(first_rows, rows_ref)
        second += pass_on(first_grads, grads_ref)
        for copy in second:
            copy.wait_recv()
        for copy in first_rows + first_grads + second:
            copy.wait_send()

    return pl.pallas_call(
        kernel,
        out_shape=(
            jax.ShapeDtypeStruct((rows, width), F32),
            jax.ShapeDtypeStruct((rows, width), BF16),
            jax.ShapeDtypeStruct((rows, LANES), F32),
            jax.ShapeDtypeStruct((rows, LANES), F32),
            jax.ShapeDtypeStruct((wide, slots, width), BF16),
            jax.ShapeDtypeStruct((wide, slots, width), BF16),
        ),
        in_specs=[VMEM] * 7,
        out_specs=(VMEM,) * 6,
        scratch_shapes=scatter_scratch(rows, width)
        + [
            pltpu.VMEM((experts - 1, slots, width), BF16),
            pltpu.VMEM((experts - 1, slots, width), BF16),
            pltpu.VMEM((2, rows, width), BF16),
            pltpu.SemaphoreType.DMA((2, 4 * experts + 3 * PARTS)),
        ],
        compiler_params=pltpu.CompilerParams(collective_id=cid, has_side_effects=True),
    )(partial, residual, gains, router, routes, cotangent, target)


def combine(
    part, row_grads, third, routed, probs, gates, gains, router, routes, cotangent, target, tokens, cid
):
    wide, slots, width = part.shape
    experts = wide // 2
    rows = third.shape[0]
    cuts = cuts_of(rows, PARTS)

    def kernel(
        part_ref,
        row_grads_ref,
        third_ref,
        routed_ref,
        probs_ref,
        gates_ref,
        gain_ref,
        router_ref,
        routes_ref,
        cot_ref,
        target_ref,
        output_ref,
        grad_ref,
        gain_grad_ref,
        router_grad_ref,
        whole_ref,
        from_part,
        from_grads,
        send_part,
        send_grads,
        back_part,
        back_grads,
        all_sems,
    ):
        bank = Bank(all_sems)
        _, near, across, _ = seq_places()
        me, half, expert, partner = wide_places()
        gather = RowGather(bank, whole_ref, cuts)
        homes = [lax.rem(expert + d, experts) for d in range(1, experts)] + [expert]
        greet((near, across), [2 * h + half for h in homes[:-1]] + [partner])

        def halves(src, into):
            copies = []
            for d, home in enumerate(homes):
                copies.append(
                    bank.remote(src.at[2 * home + 1 - half], into.at[d], "wide", partner)
                )
                copies[-1].start()
            return copies

        def homeward(copies, src, arrived, send, back):
            sent = []
            for d, home in enumerate(homes):
                copies[d].wait_recv()
                both = (src[2 * home + half].astype(F32) + arrived[d].astype(F32)).astype(BF16)
                if d == experts - 1:
                    back[expert] = both
                else:
                    send[d] = both
                    sent.append(
                        bank.remote(send.at[d], back.at[expert], "wide", 2 * home + half)
                    )
                    sent[-1].start()
            return sent

        part_halves = halves(part_ref, from_part)
        grad_halves = halves(row_grads_ref, from_grads)
        part_sent = homeward(part_halves, part_ref, from_part, send_part, back_part)
        grad_sent = homeward(
            grad_halves, row_grads_ref, from_grads, send_grads, back_grads
        )

        spot = lax.broadcasted_iota(jnp.int32, (rows, experts * slots), 1)
        picks = [(spot == target_ref[:, k : k + 1]).astype(F32) for k in range(2)]
        cot = cot_ref[...].astype(F32)
        lane = lax.broadcasted_iota(jnp.int32, (rows, LANES), 1)
        for copy in part_sent:
            copy.wait_recv()
        returned = back_part[...].reshape(experts * slots, width)
        output = third_ref[...]
        grad_probs = jnp.zeros((rows, LANES), F32)
        for k in range(2):
            picked = jnp.dot(picks[k].astype(BF16), returned, preferred_element_type=F32)
            output += gates_ref[:, k : k + 1] * picked
            grad_gate = jnp.sum(cot * picked, axis=-1, keepdims=True)
            grad_probs += jnp.where(lane == routes_ref[:, k : k + 1], grad_gate, 0.0)
        output_ref[...] = output[:tokens]
        probs = probs_ref[...]
        delta = jnp.sum(probs * grad_probs, axis=-1, keepdims=True)
        logit_grad = probs * (grad_probs - delta)
        logit_low = logit_grad.astype(BF16)
        router_grad_ref[...] = jnp.dot(
            logit_low.astype(F32).T.astype(BF16), routed_ref[...], preferred_element_type=F32
        )
        routed_grad = jnp.dot(logit_low, router_ref[...], preferred_element_type=F32)
        for copy in grad_sent:
            copy.wait_recv()
        routed_grad += jnp.dot(
            (picks[0] + picks[1]).astype(BF16),
            back_grads[...].reshape(experts * slots, width),
            preferred_element_type=F32,
        )
        grad_in, gain_grad = norm_backward(third_ref[...], gain_ref[3:4, :], routed_grad)
        gain_grad_ref[...] = gain_grad
        grad_ref[...] = cot + grad_in
        for i, (at, size) in enumerate(cuts):
            gather.send(i, grad_ref[pl.ds(at, size), :].astype(BF16))
        gather.finish()
        for copy in part_halves + grad_halves + part_sent + grad_sent:
            copy.wait_send()

    blocks = pltpu.VMEM((experts, slots, width), BF16)
    sends = pltpu.VMEM((experts - 1, slots, width), BF16)
    return pl.pallas_call(
        kernel,
        out_shape=(
            jax.ShapeDtypeStruct((tokens, width), F32),
            jax.ShapeDtypeStruct((rows, width), F32),
            jax.ShapeDtypeStruct((1, width), F32),
            jax.ShapeDtypeStruct((LANES, width), F32),
            jax.ShapeDtypeStruct((4, rows, width), BF16),
        ),
        in_specs=[VMEM] * 11,
        out_specs=(VMEM,) * 5,
        scratch_shapes=[
            blocks,
            blocks,
            sends,
            sends,
            blocks,
            blocks,
            pltpu.SemaphoreType.DMA((2, 4 * experts + 3 * PARTS)),
        ],
        compiler_params=pltpu.CompilerParams(collective_id=cid, has_side_effects=True),
    )(part, row_grads, third, routed, probs, gates, gains, router, routes, cotangent, target)


def gelu_parts(values):
    cdf = 0.5 * (1.0 + lax.erf(values * 0.5**0.5))
    density = jnp.exp(-0.5 * values * values) * 0.3989422804014327
    return values * cdf, cdf + values * density


def slot_targets(routes, fill_order, experts, capacity, slots):
    tokens = routes.shape[0]
    pair_expert = routes.reshape(-1)
    pair_key = (jnp.arange(2, dtype=jnp.int32)[None, :] * tokens + fill_order[:, None]).reshape(-1)
    same_expert = pair_expert[:, None] == pair_expert[None, :]
    earlier = pair_key[None, :] < pair_key[:, None]
    slot_rank = jnp.sum((same_expert & earlier).astype(jnp.int32), axis=1)
    target = jnp.where(slot_rank < capacity, pair_expert * slots + slot_rank, -1)
    return target.reshape(tokens, 2)


def dense(a, b, dims, dtype=BF16):
    return lax.dot_general(a, b, (dims, ((), ())), preferred_element_type=F32).astype(dtype)


def on_device(
    images,
    cotangent,
    key_mask,
    routes,
    fill_order,
    norm_gain1,
    qkv_weight1,
    proj_weight1,
    norm_gain2,
    fc_in,
    fc_out,
    norm_gain3,
    qkv_weight2,
    proj_weight2,
    norm_gain4,
    router,
    expert_in,
    expert_out,
):
    seq = lax.axis_size("seq")
    wide = lax.axis_size("wide")
    place = lax.axis_index("seq")
    tokens, width = images.shape[1:]
    rows = round_up(tokens, ROW_TILE)
    pad = rows - tokens
    total = seq * rows
    experts = wide // 2
    capacity = (5 * tokens + 2 * experts - 1) // (2 * experts)
    slots = round_up(capacity, ROW_TILE)
    span = width // seq
    heads = span // HEAD_DIM
    group = round_up(span, LANES)
    shard = width // wide
    units = fc_in.shape[1]
    unit_cut = units // (seq * wide)

    valid = jnp.pad(key_mask[0].reshape(seq, tokens) > 0, ((0, 0), (0, pad)))
    bias = jnp.where(valid, 0.0, -1e30).astype(F32)
    bias_row = bias.reshape(1, total)
    bias_col = bias.reshape(seq, rows, 1)
    target = jnp.pad(
        slot_targets(routes[0], fill_order[0], experts, capacity, slots),
        ((0, pad), (0, 0)),
        constant_values=-1,
    )
    routes_rows = jnp.pad(routes[0], ((0, pad), (0, 0)))
    cot = jnp.pad(cotangent[0], ((0, pad), (0, 0)))
    start = jnp.pad(images[0].astype(F32), ((0, pad), (0, 0)))

    tidy = shard % ROW_TILE == 0 and fc_out.shape[0] % LANES == 0 and experts == seq
    small = jnp.concatenate(
        [jnp.stack([norm_gain1, norm_gain2, norm_gain3, norm_gain4]), router.T], axis=0
    )
    if tidy:
        small = jnp.pad(small, ((0, ROW_TILE - small.shape[0]), (0, LANES - shard)))
        normed_one, gains, router_all, own_two, own_fc, wqkv_one, wproj_one = begin(
            start, small, qkv_weight1, proj_weight1, qkv_weight2, fc_in, tokens, span, group, 1
        )
        wqkv_one = wqkv_one.reshape(width, 3 * group)
    else:

        def gathered(x):
            return lax.all_gather(x, "wide", axis=0, tiled=True)

        def own_qkv(w):
            own = lax.dynamic_index_in_dim(w.reshape(shard, 3, seq, span), place, 2, keepdims=False)
            own = jnp.pad(own, ((0, 0), (0, 0), (0, group - span)))
            return gathered(own.reshape(shard, 3 * group))

        def own_proj(w):
            own = lax.dynamic_slice_in_dim(gathered(w), place * span, span, 0)
            return own.reshape(2, span // 2, width)

        small = lax.all_gather(small, "wide", axis=0)
        small = small.transpose(1, 0, 2).reshape(4 + experts, width)
        gains = small[:4].astype(F32)
        router_all = jnp.pad(small[4:], ((0, LANES - experts), (0, 0)))
        wqkv_one = own_qkv(qkv_weight1)
        wproj_one = own_proj(proj_weight1)
        w_in = gathered(
            lax.dynamic_index_in_dim(
                fc_in.reshape(shard, wide, seq, unit_cut), place, 2, keepdims=False
            ).reshape(shard, wide * unit_cut)
        )
        w_out = gathered(lax.dynamic_slice_in_dim(fc_out, place * unit_cut, unit_cut, 0))
        wqkv_two = own_qkv(qkv_weight2)
        wproj_two = own_proj(proj_weight2)
        normed_one = spread_norm(start, gains, tokens, 1)

    tasks = [spread_task(own_fc)] if tidy else []
    qkv_one, lse_one, mixed_one, part, *came = attend_forward(
        normed_one, wqkv_one, wproj_one, bias_row, heads, 2 if tidy else None, tasks
    )
    if tidy:
        w_in = came[0].reshape(width, wide * unit_cut)
        cut = LANES // seq
        tasks = [
            spread_task(
                fc_out.reshape(-1, LANES, width),
                lambda ref: ref.at[:, pl.ds(lax.axis_index("seq") * cut, cut)],
                (fc_out.shape[0] // LANES, cut, width),
            )
        ]
    first, normed_two, *came = join_forward(part, start, gains, 1, tokens, 3, tasks)
    if tidy:
        w_out = came[0].reshape(-1, width)
    flat_two = normed_two.reshape(total, width)
    pre = dense(flat_two, w_in, ((1,), (0,)), F32)
    hidden, slope = gelu_parts(pre)
    hidden, slope = hidden.astype(BF16), slope.astype(BF16)
    part = dense(hidden, w_out, ((1,), (0,))).reshape(seq, rows, width)
    tasks = [spread_task(own_two), root_spread_task(proj_weight2)] if tidy else []
    second, normed_three, *came = join_forward(part, first, gains, 2, tokens, 4, tasks)
    if tidy:
        wqkv_two = came[0].reshape(width, 3 * group)
        wproj_two = came[1]
    qkv_two, lse_two, mixed_two, part = attend_forward(
        normed_three, wqkv_two, wproj_two, bias_row, heads
    )
    third, routed, probs, gates, got_rows, got_grads = dispatch(
        part, second, gains, router_all, routes_rows, cot, target.T, tokens, slots, 5
    )
    got_rows = got_rows.reshape(wide * slots, width)
    got_grads = got_grads.reshape(wide * slots, width)
    pre = dense(got_rows, expert_in[0], ((1,), (0,)), F32)
    e_hidden, e_slope = gelu_parts(pre)
    e_hidden = e_hidden.astype(BF16)
    e_part = dense(e_hidden, expert_out[0], ((1,), (0,)))
    e_pre = (dense(got_grads, expert_out[0], ((1,), (1,)), F32) * e_slope).astype(BF16)
    e_rows = dense(e_pre, expert_in[0], ((1,), (1,)))
    output, grad, gain4_grad, router_grad, branch = combine(
        e_part.reshape(wide, slots, width),
        e_rows.reshape(wide, slots, width),
        third,
        routed,
        probs,
        gates,
        gains,
        router_all,
        routes_rows,
        cot,
        target,
        tokens,
        6,
    )
    e_out_grad = dense(e_hidden, got_grads, ((0,), (0,)))
    e_in_grad = dense(got_rows, e_pre, ((0,), (0,)))

    def qkv_terms(normed, grad_qkv):
        return dense(normed.reshape(total, width), grad_qkv.reshape(total, 3 * group), ((0,), (0,)))

    def proj_terms(mixed, branch):
        return dense(mixed.reshape(total, group), branch.reshape(total, width), ((0,), (0,)))[:span]

    def reduced(terms):
        own = lax.psum_scatter(terms, "wide", scatter_dimension=0, tiled=True)
        return lax.all_gather(own, "seq", axis=0).astype(F32)

    def attention_grads(gq, gp):
        gq = gq.reshape(width, 3, group)[:, :, :span].reshape(width, 3 * span)
        gp = lax.all_to_all(gp, "seq", split_axis=1, concat_axis=0, tiled=True)
        whole = reduced(jnp.concatenate([gq, gp], axis=1))
        gq = whole[:, :, : 3 * span].reshape(seq, shard, 3, span).transpose(1, 2, 0, 3)
        gp = whole[:, :, 3 * span :].transpose(1, 0, 2)
        return gq.reshape(shard, 3 * width), gp.reshape(shard, width)

    grad_qkv, part = attend_backward(
        branch, qkv_two, lse_two, mixed_two, wqkv_two, wproj_two, bias_col, heads
    )
    qkv_two_terms = qkv_terms(normed_three, grad_qkv)
    proj_two_terms = proj_terms(mixed_two, branch)
    tasks = []
    if tidy:
        tasks = [
            reduce_task(qkv_two_terms.reshape(wide, shard, 3 * group)),
            root_reduce_task(proj_two_terms.reshape(2, shard, width)),
        ]
    grad, gain3_grad, branch, *came = join_backward(
        part, second, gains, 2, grad, tokens, 7, tasks
    )
    if tidy:
        qkv_two_own, proj_two_own = came
    branch_flat = branch.reshape(total, width)
    pre_grad = (dense(branch_flat, w_out, ((1,), (1,)), F32) * slope).astype(BF16)
    part = dense(pre_grad, w_in, ((1,), (1,))).reshape(seq, rows, width)
    fc_in_terms = dense(flat_two, pre_grad, ((0,), (0,)))
    fc_out_terms = dense(hidden, branch_flat, ((0,), (0,)))
    tasks = [reduce_task(fc_in_terms.reshape(wide, shard, -1))] if tidy else []
    grad, gain2_grad, branch, *came = join_backward(
        part, first, gains, 1, grad, tokens, 8, tasks
    )
    tasks = []
    if tidy:
        tasks = [
            reduce_task(fc_out_terms.reshape(wide, -1, width)),
            block_gather_task(came[0]),
            block_gather_task(qkv_two_own),
        ]
    grad_qkv, part, *came = attend_backward(
        branch,
        qkv_one,
        lse_one,
        mixed_one,
        wqkv_one,
        wproj_one,
        bias_col,
        heads,
        9 if tidy else None,
        tasks,
    )
    qkv_one_terms = qkv_terms(normed_one, grad_qkv)
    proj_one_terms = proj_terms(mixed_one, branch)
    others = [gain2_grad, gain3_grad, gain4_grad, router_grad[:experts]]
    if tidy:
        image_grad, small_own, qkv_one_all, fc_out_all, proj_one_own = close(
            part,
            start,
            gains,
            grad,
            jnp.concatenate(others, axis=0),
            qkv_one_terms.reshape(wide, shard, 3 * group),
            proj_one_terms.reshape(2, shard, width),
            came[0],
            tokens,
            10,
        )
        small_own = small_own[:, :shard]
        qkv1_grad, qkv2_grad, fc_in_grad, fc_out_grad, proj1_grad, proj2_grad = assemble(
            qkv_one_all, came[2], came[1], fc_out_all, proj_one_own, proj_two_own, span, group
        )
    else:
        image_grad, gain1_grad = close_plain(part, start, gains, grad, tokens, 10)
        qkv1_grad, proj1_grad = attention_grads(qkv_one_terms, proj_one_terms)
        qkv2_grad, proj2_grad = attention_grads(qkv_two_terms, proj_two_terms)
        fc_whole = reduced(jnp.concatenate([fc_in_terms, fc_out_terms], axis=1))
        fc_in_grad = fc_whole[:, :, : wide * unit_cut].reshape(seq, shard, wide, unit_cut)
        fc_in_grad = fc_in_grad.transpose(1, 2, 0, 3).reshape(shard, units)
        fc_out_grad = fc_whole[:, :, wide * unit_cut :].reshape(seq * unit_cut, width)
        small_own = lax.psum(jnp.concatenate([gain1_grad] + others, axis=0), ("seq", "wide"))
        small_own = lax.dynamic_slice_in_dim(
            small_own, lax.axis_index("wide") * shard, shard, 1
        )
    e_in_all = lax.psum(e_in_grad, "seq").astype(F32)
    e_out_all = lax.psum(e_out_grad, "seq").astype(F32)
    return (
        output[None],
        image_grad[None],
        small_own[0],
        qkv1_grad,
        proj1_grad,
        small_own[1],
        fc_in_grad,
        fc_out_grad,
        small_own[2],
        qkv2_grad,
        proj2_grad,
        small_own[3],
        small_own[4 : 4 + experts].T,
        e_in_all[None],
        e_out_all[None],
    )


def solution(mesh):
    placed = (
        P("wide", "seq", None),
        P("wide", "seq", None),
        P("wide", None),
        P("wide", "seq", None),
        P("wide", "seq"),
        P("wide"),
        P("wide", None),
        P("wide", None),
        P("wide"),
        P("wide", None),
        P("wide", None),
        P("wide"),
        P("wide", None),
        P("wide", None),
        P("wide"),
        P("wide", None),
        P("wide", None, None),
        P("wide", None, None),
    )
    return jax.shard_map(
        on_device,
        mesh=mesh,
        in_specs=placed,
        out_specs=(
            P("wide", "seq", None),
            P("wide", "seq", None),
            P("wide"),
            P("wide", None),
            P("wide", None),
            P("wide"),
            P("wide", None),
            P("wide", None),
            P("wide"),
            P("wide", None),
            P("wide", None),
            P("wide"),
            P("wide", None),
            P("wide", None, None),
            P("wide", None, None),
        ),
        check_vma=False,
    )
```
